32 devices in a mesh: grp: 2 (over x), seq: 16 (over z, y, core).
Axes of the slice: x: 2, y: 2, z: 4, core: 2. Of those that a mesh axis runs over, the one named last changes fastest.
Arguments:
- queries: bfloat16 [8, 4096], P('grp', 'seq'), parts along dimension 0, may hold values from -40 to 40
- gate_logits: float32 [8, 64], P('grp'), parts along dimension 0, may hold values from -6 to 6
- kv_pool: bfloat16 [512, 128, 2048], P(('grp', 'seq')), parts along dimension 0, may hold values from -6 to 6
- page_table: int32 [8, 64], P('grp'), parts along dimension 0, may hold values from 0 to 255, as said below
- selected: int32 [8, 8, 16], P('grp'), parts along dimension 0, may hold values from 0 to 63, as said below
- lengths: int32 [8], P('grp'), parts along dimension 0, may hold values from 4096 to 8192, as said below
Outputs:
- attended: bfloat16 [8, 4096], P('grp', 'seq'), parts along dimension 0
The draws below stay inside these ranges and needn't reach their ends.
There are 2 independent parts, one for each index of `grp`. The reference program is written for one: setup_inputs(seed, part) draws one part's arguments, and reference() takes and returns one part's arrays. A program takes and returns all parts, laid end to end along the dimension named above; each array names one. Nothing has to cross between parts.
Inputs may be any that keep to these rules, and one draw needn't show every extreme that they name: `page_table`: a one-to-one map of the 4 x 64 pages onto the pool slots; each aligned run of 2 pages of a request lies in 2 consecutive slots starting at a multiple of 2. `lengths`: some request in every draw has length 8192. `selected`: for each request and key-value head, 16 different pages, all among the request's last 32 live pages, the last live page among them.
All inputs are finite; a program needn't handle non-finite values.
Results may differ from the reference program's by a relative error of at most 0.0039.
Values may be sent and summed in bfloat16 or wider, within the bound.
A program may use at most 64 MiB of HBM per device.

```python
import math
import jax
import jax.numpy as jnp
from jax import lax

QUERY_HEADS = 32
KV_HEADS = 8
HEAD_DIM = 128
PAGE_LEN = 128
TOP_PAGES = 16
RECENT_PAGES = 32
RUN_PAGES = 2
REQUESTS = 4
CTX_PAGES = 64
POOL_SLOTS = 256


def one_order(one_key):
    return jax.random.permutation(one_key, CTX_PAGES)


def layout_tables(key):
    key_len = jax.random.fold_in(key, 11)
    key_pick = jax.random.fold_in(key, 12)
    key_runs = jax.random.fold_in(key, 13)
    key_sel = jax.random.fold_in(key, 14)
    longest = CTX_PAGES * PAGE_LEN
    drawn_len = jax.random.randint(key_len, (REQUESTS,), RECENT_PAGES * PAGE_LEN, longest + 1, dtype=jnp.int32)
    pick_row = jax.random.randint(key_pick, (), 0, REQUESTS, dtype=jnp.int32)
    lengths = jnp.where(jnp.arange(REQUESTS, dtype=jnp.int32) == pick_row, longest, drawn_len).astype(jnp.int32)
    run_count = REQUESTS * CTX_PAGES // RUN_PAGES
    run_order = jax.random.permutation(key_runs, run_count).astype(jnp.int32)
    flat_index = jnp.arange(REQUESTS * CTX_PAGES, dtype=jnp.int32)
    page_map = (run_order[flat_index // RUN_PAGES] * RUN_PAGES + flat_index % RUN_PAGES).reshape(REQUESTS, CTX_PAGES).astype(jnp.int32)
    last_page = (lengths - 1) // PAGE_LEN
    sel_keys = jax.random.split(key_sel, REQUESTS * KV_HEADS)
    orders = jax.vmap(one_order)(sel_keys).astype(jnp.int32).reshape(REQUESTS, KV_HEADS, CTX_PAGES)
    page_ids = jnp.arange(CTX_PAGES, dtype=jnp.int32)[None, None, :]
    last_col = last_page[:, None, None]
    recent = (page_ids <= last_col) & (page_ids > last_col - RECENT_PAGES)
    scores = jnp.where(page_ids == last_col, -1, jnp.where(recent, orders, orders + 2 * CTX_PAGES)).astype(jnp.int32)
    chosen = lax.top_k(-scores, TOP_PAGES)[1].astype(jnp.int32)
    return (lengths, page_map, chosen)


def draw_lengths(key, part):
    return layout_tables(key)[0]


def draw_page_table(key, part):
    return layout_tables(key)[1]


def draw_selected(key, part):
    return layout_tables(key)[2]


def draw_kv_pool(key, part):
    lengths, page_map, chosen = layout_tables(key)
    kv_width = KV_HEADS * HEAD_DIM
    key_page = jax.random.fold_in(key, 21)
    key_noise = jax.random.fold_in(key, 22)
    common = jax.random.normal(key_page, (POOL_SLOTS, 1, 2 * kv_width), jnp.float32)
    noise = jax.random.normal(key_noise, (POOL_SLOTS, PAGE_LEN, 2 * kv_width), jnp.float32)
    pool = jnp.clip(0.8 * common + 0.6 * noise, -6.0, 6.0)
    return pool.astype(jnp.bfloat16)


def draw_queries(key, part):
    key_query = jax.random.fold_in(key, 31)
    values = jnp.clip(2.0 * jax.random.normal(key_query, (REQUESTS, QUERY_HEADS * HEAD_DIM), jnp.float32), -12.0, 12.0)
    return values.astype(jnp.bfloat16)


def scatter_about(rng, dims, width, most, held_as=jnp.bfloat16):
    return jnp.clip(width * jax.random.normal(rng, dims, jnp.float32), -most, most).astype(held_as)


def setup_inputs(seed: int = 0, part: int = 0) -> dict:
    splits = jax.random.split(jax.random.key(seed), 7)
    own_keys = jax.random.split(jax.random.fold_in(splits[6], part), 7)
    return {
        "queries": draw_queries(jax.random.fold_in(jax.random.fold_in(splits[6], part), 71), part),
        "gate_logits": scatter_about(own_keys[1], (REQUESTS, 2 * QUERY_HEADS), 1.5, 6.0, jnp.float32),
        "kv_pool": draw_kv_pool(jax.random.fold_in(jax.random.fold_in(splits[6], part), 71), part),
        "page_table": draw_page_table(jax.random.fold_in(jax.random.fold_in(splits[6], part), 71), part),
        "selected": draw_selected(jax.random.fold_in(jax.random.fold_in(splits[6], part), 71), part),
        "lengths": draw_lengths(jax.random.fold_in(jax.random.fold_in(splits[6], part), 71), part),
    }


neg_big = -1e+30

def reference(queries, gate_logits, kv_pool, page_table, selected, lengths):
    group_size = QUERY_HEADS // KV_HEADS
    kv_width = KV_HEADS * HEAD_DIM
    score_scale = 1.0 / math.sqrt(HEAD_DIM)
    highest = lax.Precision.HIGHEST
    gate_all = jax.nn.sigmoid(gate_logits.astype(jnp.float32))

    def one_request(request):
        query_rows = queries[request].reshape(KV_HEADS, group_size, HEAD_DIM).astype(jnp.float32)
        page_rows = kv_pool[page_table[request]]
        key_rows = page_rows[:, :, :kv_width].reshape(CTX_PAGES, PAGE_LEN, KV_HEADS, HEAD_DIM).astype(jnp.float32)
        value_rows = page_rows[:, :, kv_width:].reshape(CTX_PAGES, PAGE_LEN, KV_HEADS, HEAD_DIM).astype(jnp.float32)
        length = lengths[request]
        page_ids = jnp.arange(CTX_PAGES, dtype=jnp.int32)
        position = page_ids[:, None] * PAGE_LEN + jnp.arange(PAGE_LEN, dtype=jnp.int32)[None, :]
        is_valid = position < length
        valid_f = is_valid.astype(jnp.float32)
        is_live = page_ids * PAGE_LEN < length
        counts = jnp.maximum(lax.optimization_barrier(jnp.sum(valid_f, axis=1)), 1.0)
        summary_keys = (jnp.einsum('pt,ptkd->pkd', valid_f, key_rows, precision=highest) / counts[:, None, None]).astype(jnp.bfloat16)
        summary_keys = lax.optimization_barrier(summary_keys).astype(jnp.float32)
        summary_values = (jnp.einsum('pt,ptkd->pkd', valid_f, value_rows, precision=highest) / counts[:, None, None]).astype(jnp.bfloat16)
        summary_values = lax.optimization_barrier(summary_values).astype(jnp.float32)
        coarse = jnp.einsum('kgd,pkd->kgp', query_rows, summary_keys, precision=highest) * score_scale
        live_mask = is_live[None, None, :]
        coarse_masked = jnp.where(live_mask, coarse, neg_big)
        coarse_top = lax.optimization_barrier(jnp.max(coarse_masked, axis=2))
        coarse_wt = jnp.where(live_mask, jnp.exp(coarse_masked - coarse_top[..., None]), 0.0)
        coarse_out = jnp.einsum('kgp,pkd->kgd', coarse_wt, summary_values, precision=highest) / lax.optimization_barrier(jnp.sum(coarse_wt, axis=2))[..., None]
        fine_scores = jnp.einsum('kgd,ptkd->pkgt', query_rows, key_rows, precision=highest) * score_scale
        token_mask = is_valid[:, None, None, :]
        fine_masked = jnp.where(token_mask, fine_scores, neg_big)
        page_max = lax.optimization_barrier(jnp.max(fine_masked, axis=3))
        page_wt = jnp.where(token_mask, jnp.exp(fine_masked - page_max[..., None]), 0.0).astype(jnp.bfloat16)
        page_wt = lax.optimization_barrier(page_wt).astype(jnp.float32)
        page_sum = lax.optimization_barrier(jnp.sum(page_wt, axis=3))
        page_num = jnp.einsum('pkgt,ptkd->pkgd', page_wt, value_rows, precision=highest)
        chosen = jnp.any(selected[request][:, :, None] == page_ids[None, None, :], axis=1)
        chosen_full = chosen.T[:, :, None]
        sel_masked = jnp.where(chosen_full, page_max, neg_big)
        fine_top = lax.optimization_barrier(jnp.max(sel_masked, axis=0))
        fine_wt = jnp.where(chosen_full, jnp.exp(sel_masked - fine_top[None]), 0.0)
        fine_den = lax.optimization_barrier(jnp.sum(fine_wt * page_sum, axis=0))
        fine_out = jnp.einsum('pkg,pkgd->kgd', fine_wt, page_num, precision=highest) / fine_den[..., None]
        gate_row = gate_all[request]
        coarse_gate = gate_row[:QUERY_HEADS].reshape(KV_HEADS, group_size)
        fine_gate = gate_row[QUERY_HEADS:].reshape(KV_HEADS, group_size)
        mixed = coarse_gate[..., None] * coarse_out + fine_gate[..., None] * fine_out
        return mixed.reshape(QUERY_HEADS * HEAD_DIM).astype(jnp.bfloat16)
    return lax.map(one_request, jnp.arange(REQUESTS, dtype=jnp.int32))
```

```python
import functools
import math

import jax
import jax.numpy as jnp
from jax import lax
from jax.experimental import pallas as pl
from jax.experimental.pallas import tpu as pltpu
from jax.sharding import PartitionSpec as P

HEAD_DIM = 128


neg_big = -1e30


def joined(part, axis, combine):
    gathered = jax.tree.map(lambda a: lax.all_gather(a, axis), part)

    def take(source):
        return jax.tree.map(lambda a: lax.dynamic_index_in_dim(a, source, 0, False), gathered)

    return lax.fori_loop(
        1, lax.axis_size(axis), lambda source, state: combine(state, take(source)), take(0)
    )


def merge_pair(left, right):
    merged = ()
    for offset in (0, 3):
        row_top = jnp.maximum(left[offset], right[offset])
        left_scale = jnp.exp(left[offset] - row_top)
        right_scale = jnp.exp(right[offset] - row_top)
        merged = merged + (
            row_top,
            left[offset + 1] * left_scale + right[offset + 1] * right_scale,
            left[offset + 2] * left_scale[..., None] + right[offset + 2] * right_scale[..., None],
        )
    return merged


def per_device_plain(queries, gate_logits, kv_pool, page_table, selected, lengths):
    slot_count, page_len, double_width = kv_pool.shape
    kv_width = double_width // 2
    kv_heads = kv_width // HEAD_DIM
    requests = page_table.shape[0]
    ctx_pages = page_table.shape[1]
    col_count = queries.shape[1]
    highest = lax.Precision.HIGHEST
    all_queries = lax.all_gather(queries, "seq", axis=1, tiled=True)
    head_count = all_queries.shape[1] // HEAD_DIM
    group_size = head_count // kv_heads
    score_scale = 1.0 / math.sqrt(HEAD_DIM)
    first_slot = lax.axis_index("seq") * slot_count
    slot_ids = first_slot + jnp.arange(slot_count, dtype=jnp.int32)
    slot_match = page_table[:, :, None] == slot_ids[None, None, :]
    owner_hot = jnp.any(slot_match, axis=1)
    page_index = jnp.arange(ctx_pages, dtype=jnp.int32)
    page_of = jnp.sum(jnp.where(slot_match, page_index[None, :, None], 0), axis=(0, 1))
    slot_len = jnp.sum(jnp.where(owner_hot, lengths[:, None], 0), axis=0)
    owner_rows = jnp.dot(
        owner_hot.T.astype(jnp.bfloat16), all_queries, preferred_element_type=jnp.float32
    ).astype(jnp.bfloat16)
    slot_queries = owner_rows.reshape(slot_count, kv_heads, group_size, HEAD_DIM)
    key_rows = kv_pool[:, :, :kv_width].reshape(slot_count, page_len, kv_heads, HEAD_DIM)
    value_rows = kv_pool[:, :, kv_width:].reshape(slot_count, page_len, kv_heads, HEAD_DIM)
    position = page_of[:, None] * page_len + jnp.arange(page_len, dtype=jnp.int32)[None, :]
    is_valid = position < slot_len[:, None]
    is_live = page_of * page_len < slot_len
    valid_bf = is_valid.astype(jnp.bfloat16)
    counts = jnp.maximum(jnp.sum(is_valid.astype(jnp.float32), axis=1), 1.0)
    summary_keys = (
        jnp.einsum("st,stkd->skd", valid_bf, key_rows, preferred_element_type=jnp.float32)
        / counts[:, None, None]
    ).astype(jnp.bfloat16)
    summary_values = (
        jnp.einsum("st,stkd->skd", valid_bf, value_rows, preferred_element_type=jnp.float32)
        / counts[:, None, None]
    ).astype(jnp.bfloat16)
    coarse = (
        jnp.einsum("skgd,skd->skg", slot_queries, summary_keys, preferred_element_type=jnp.float32)
        * score_scale
    )
    coarse_mask = owner_hot[:, :, None, None] & is_live[None, :, None, None]
    coarse_masked = jnp.where(coarse_mask, coarse[None], neg_big)
    coarse_top = jnp.max(coarse_masked, axis=1)
    coarse_wt = jnp.where(coarse_mask, jnp.exp(coarse_masked - coarse_top[:, None]), 0.0)
    coarse_sum = jnp.sum(coarse_wt, axis=1)
    coarse_num = jnp.einsum(
        "rskg,skd->rkgd", coarse_wt, summary_values.astype(jnp.float32), precision=highest
    )
    fine_scores = (
        jnp.einsum("skgd,stkd->skgt", slot_queries, key_rows, preferred_element_type=jnp.float32)
        * score_scale
    )
    token_mask = is_valid[:, None, None, :]
    fine_masked = jnp.where(token_mask, fine_scores, neg_big)
    page_max = jnp.max(fine_masked, axis=3)
    page_wt = jnp.where(token_mask, jnp.exp(fine_masked - page_max[..., None]), 0.0).astype(
        jnp.bfloat16
    )
    page_sum = jnp.sum(page_wt.astype(jnp.float32), axis=3)
    page_num = jnp.einsum(
        "skgt,stkd->skgd", page_wt, value_rows, preferred_element_type=jnp.float32
    )
    page_hit = selected[:, None, :, :] == page_of[None, :, None, None]
    chosen = jnp.any(page_hit, axis=3) & owner_hot[:, :, None]
    chosen_full = chosen[..., None]
    sel_masked = jnp.where(chosen_full, page_max[None], neg_big)
    fine_top = jnp.max(sel_masked, axis=1)
    fine_wt = jnp.where(chosen_full, jnp.exp(sel_masked - fine_top[:, None]), 0.0)
    fine_sum = jnp.sum(fine_wt * page_sum[None], axis=1)
    fine_num = jnp.einsum("rskg,skgd->rkgd", fine_wt, page_num, precision=highest)
    gate_all = jax.nn.sigmoid(gate_logits)
    start_col = lax.axis_index("seq") * col_count
    coarse_gate = lax.dynamic_slice_in_dim(
        jnp.repeat(gate_all[:, :head_count], HEAD_DIM, axis=1), start_col, col_count, 1
    )
    fine_gate = lax.dynamic_slice_in_dim(
        jnp.repeat(gate_all[:, head_count:], HEAD_DIM, axis=1), start_col, col_count, 1
    )
    merged = joined(
        (coarse_top, coarse_sum, coarse_num, fine_top, fine_sum, fine_num), "seq", merge_pair
    )
    coarse_full = (merged[2] / merged[1][..., None]).reshape(requests, head_count * HEAD_DIM)
    fine_full = (merged[5] / merged[4][..., None]).reshape(requests, head_count * HEAD_DIM)
    coarse_cols = lax.dynamic_slice_in_dim(coarse_full, start_col, col_count, 1)
    fine_cols = lax.dynamic_slice_in_dim(fine_full, start_col, col_count, 1)
    return (coarse_gate * coarse_cols + fine_gate * fine_cols).astype(jnp.bfloat16)


RUN = 2
MESH = pl.DeviceIdType.MESH
F32 = jnp.float32
BF16 = jnp.bfloat16


def fused_kernel(
    n, q_hbm, gate_hbm, kv_hbm, pt_hbm, sel_hbm, len_hbm, out_ref,
    kv_buf, q_all, gate_v, pt_v, sel_v, len_s, q_even, gather_f, send_buf, recv_buf,
    kv_sem, in_sem, q_send, q_recv, p_send, p_recv,
):
    me = lax.axis_index("seq")
    slots, page_len, width = kv_buf.shape
    kv_width = width // 2
    kv_heads = kv_width // HEAD_DIM
    runs = slots // RUN
    span = RUN * page_len
    requests, ctx = pt_v.shape
    per_dev = q_all.shape[2] // HEAD_DIM
    heads = per_dev * n
    group = heads // kv_heads
    scale = math.log2(math.e) / math.sqrt(HEAD_DIM)

    def load_run(j):
        return pltpu.make_async_copy(
            kv_hbm.at[pl.ds(j * RUN, RUN)], kv_buf.at[pl.ds(j * RUN, RUN)], kv_sem.at[j]
        )

    small = [
        pltpu.make_async_copy(q_hbm, q_all.at[me], in_sem.at[0]),
        pltpu.make_async_copy(pt_hbm, pt_v, in_sem.at[1]),
        pltpu.make_async_copy(len_hbm, len_s, in_sem.at[2]),
        pltpu.make_async_copy(sel_hbm, sel_v, in_sem.at[3]),
        pltpu.make_async_copy(gate_hbm, gate_v, in_sem.at[4]),
    ]
    barrier = pltpu.get_barrier_semaphore()
    peers = [lax.rem(me + step, n) for step in range(1, n)]
    for peer in peers:
        pl.semaphore_signal(barrier, inc=1, device_id={"seq": peer}, device_id_type=MESH)
    for copy in small:
        copy.start()
    for j in range(runs):
        load_run(j).start()
    small[0].wait()
    pl.semaphore_wait(barrier, n - 1)

    def q_copy(slot, peer):
        return pltpu.make_async_remote_copy(
            src_ref=q_all.at[slot], dst_ref=q_all.at[slot], send_sem=q_send.at[peer],
            recv_sem=q_recv.at[slot], device_id={"seq": peer}, device_id_type=MESH,
        )

    for peer in peers:
        q_copy(me, peer).start()
    for copy in small[1:]:
        copy.wait()

    table = pt_v[...]
    row_id = lax.broadcasted_iota(jnp.int32, (requests, ctx), 0)
    col_f = lax.broadcasted_iota(jnp.int32, (requests, ctx), 1).astype(F32)
    len_grid = jnp.zeros((requests, ctx), F32)
    for r in range(requests):
        len_grid = jnp.where(row_id == r, len_s[r].astype(F32), len_grid)
    head_row = lax.broadcasted_iota(jnp.int32, (heads, 1), 0)
    head_id = lax.rem(head_row, n) * per_dev + head_row // n
    kv_row = head_id // group
    chosen_ids = []
    for r in range(requests):
        ids = sel_v[r].astype(F32)
        wide = jnp.zeros((heads, ids.shape[1]), F32)
        for k in range(kv_heads):
            wide = jnp.where(kv_row == k, ids[k : k + 1, :], wide)
        chosen_ids.append(wide)
    lane = lax.broadcasted_iota(jnp.int32, (1, span), 1)
    lane_f = lane.astype(F32)
    hot, valid, fine_ok, live, count = [], [], [], [], []
    for j in range(runs):
        match = table == me * slots + j * RUN
        page = jnp.sum(jnp.where(match, col_f, 0.0), axis=(0, 1), keepdims=True)
        length = jnp.sum(jnp.where(match, len_grid, 0.0), axis=(0, 1), keepdims=True)
        owner = jnp.max(jnp.where(match, 1.0, 0.0), axis=1, keepdims=True)
        hot_j = [owner[r : r + 1, :] for r in range(requests)]
        ids = chosen_ids[0] * hot_j[0]
        for r in range(1, requests):
            ids = ids + chosen_ids[r] * hot_j[r]
        valid_j = jnp.where(page * page_len + lane_f < length, 1.0, 0.0)
        ok = jnp.zeros((heads, span), F32)
        live_j, count_j = [], []
        for e in range(RUN):
            hit = jnp.max(jnp.where(ids == page + e, 1.0, 0.0), axis=1, keepdims=True)
            ok = jnp.where(lane // page_len == e, hit, ok)
            left = length - (page + e) * page_len
            live_j.append(jnp.where(left > 0.0, 1.0, 0.0))
            count_j.append(jnp.clip(left, 1.0, float(page_len)))
        hot.append(hot_j)
        valid.append(valid_j)
        fine_ok.append(ok * valid_j)
        live.append(live_j)
        count.append(count_j)

    for step, peer in enumerate(peers):
        q_copy(peer, peer).wait_recv()
    for src in range(n):
        rows = q_all[src].astype(F32)
        for w in range(per_dev):
            q_even[w, src * requests : (src + 1) * requests, :] = rows[
                :, w * HEAD_DIM : (w + 1) * HEAD_DIM
            ]
    q_rows = [
        jnp.concatenate(
            [q_even[w, pl.ds(r, n, stride=requests), :] for w in range(per_dev)], axis=0
        )
        for r in range(requests)
    ]

    fine_m, fine_l, fine_n, coarse_s, coarse_v = [], [], [], [], []
    valid_rows = 16
    row16 = lax.broadcasted_iota(jnp.int32, (valid_rows, span), 0)
    for j in range(runs):
        q_j = q_rows[0] * hot[j][0]
        for r in range(1, requests):
            q_j = q_j + q_rows[r] * hot[j][r]
        q_bd = jnp.concatenate(
            [jnp.where(kv_row == k, q_j, 0.0) for k in range(kv_heads)], axis=1
        ).astype(BF16)
        load_run(j).wait()
        keys = kv_buf[j * RUN : (j + 1) * RUN, :, :kv_width].reshape(span, kv_width)
        vals = kv_buf[j * RUN : (j + 1) * RUN, :, kv_width:].reshape(span, kv_width)
        scores = lax.dot_general(
            q_bd, keys, (((1,), (1,)), ((), ())), preferred_element_type=F32
        ) * scale
        ok = fine_ok[j] > 0.0
        masked = jnp.where(ok, scores, neg_big)
        top = jnp.max(masked, axis=1, keepdims=True)
        wt = jnp.where(ok, jnp.exp2(masked - top), 0.0).astype(BF16)
        fine_m.append(top)
        fine_l.append(jnp.sum(wt.astype(F32), axis=1, keepdims=True))
        shown = scores * valid[j]
        page_rows = jnp.where(lane // page_len == row16, valid[j], 0.0).astype(BF16)
        mixed = lax.dot_general(
            jnp.concatenate([wt, page_rows], axis=0), vals, (((1,), (0,)), ((), ())),
            preferred_element_type=F32,
        )
        num = mixed[:heads, :HEAD_DIM]
        for k in range(1, kv_heads):
            num = jnp.where(kv_row == k, mixed[:heads, k * HEAD_DIM : (k + 1) * HEAD_DIM], num)
        fine_n.append(num)
        for e in range(RUN):
            mean = jnp.sum(
                shown[:, e * page_len : (e + 1) * page_len], axis=1, keepdims=True
            ) / count[j][e]
            coarse_s.append(jnp.where(live[j][e] > 0.0, mean, neg_big))
            sv = (mixed[heads + e : heads + e + 1, :] / count[j][e]).astype(BF16).astype(F32)
            wide = jnp.broadcast_to(sv[:, :HEAD_DIM], (heads, HEAD_DIM))
            for k in range(1, kv_heads):
                wide = jnp.where(kv_row == k, sv[:, k * HEAD_DIM : (k + 1) * HEAD_DIM], wide)
            coarse_v.append(wide)

    unit = 2 * per_dev * requests
    lane_row = lax.broadcasted_iota(jnp.int32, (heads, HEAD_DIM), 1)

    def put(kind, r, top, total, num):
        top_b = top.astype(BF16).astype(F32)
        high = total.astype(BF16).astype(F32)
        stat = jnp.where(lane_row == 0, top_b, jnp.where(lane_row == 1, high, total - high))
        for w in range(per_dev):
            row = kind * per_dev * requests + w * requests + r
            gather_f[pl.ds(row, n, stride=2 * unit), :] = num[w * n : (w + 1) * n]
            gather_f[pl.ds(unit + row, n, stride=2 * unit), :] = stat[w * n : (w + 1) * n]

    for r in range(requests):
        for kind in range(2):
            if kind == 0:
                tops = coarse_s
                owner = [hot[i // RUN][r] for i in range(slots)]
            else:
                tops = fine_m
                owner = [hot[j][r] for j in range(runs)]
            held = [jnp.where(o > 0.0, t, neg_big) for o, t in zip(owner, tops)]
            top = functools.reduce(jnp.maximum, held)
            top = top.astype(BF16).astype(F32)
            total = jnp.zeros((heads, 1), F32)
            num = jnp.zeros((heads, HEAD_DIM), F32)
            for i, h in enumerate(held):
                weight = jnp.where(h > 0.5 * neg_big, jnp.exp2(h - top), 0.0)
                if kind == 0:
                    total = total + weight
                    num = num + weight * coarse_v[i]
                else:
                    total = total + weight * fine_l[i]
                    num = num + weight * fine_n[i]
            put(kind, r, top, total, num)
    for d in range(n):
        send_buf[d] = gather_f[d * 2 * unit : (d + 1) * 2 * unit, :].astype(BF16)

    def p_copy(slot, peer):
        return pltpu.make_async_remote_copy(
            src_ref=send_buf.at[peer], dst_ref=recv_buf.at[slot], send_sem=p_send.at[peer],
            recv_sem=p_recv.at[slot], device_id={"seq": peer}, device_id_type=MESH,
        )

    for peer in peers:
        p_copy(me, peer).start()
    recv_buf[me] = send_buf[me]
    gates = jax.nn.sigmoid(gate_v[...])
    gate_lane = lax.broadcasted_iota(jnp.int32, gates.shape, 1)
    gate_col = [
        [
            jnp.sum(
                jnp.where(gate_lane == kind * heads + me * per_dev + w, gates, 0.0),
                axis=1, keepdims=True,
            )
            for w in range(per_dev)
        ]
        for kind in range(2)
    ]
    for peer in peers:
        p_copy(peer, peer).wait_recv()
    stats = [recv_buf[src, unit:, :].astype(F32) for src in range(n)]
    tops = [s[:, 0:1] for s in stats]
    top = functools.reduce(jnp.maximum, tops)
    total = jnp.zeros((unit, 1), F32)
    num = jnp.zeros((unit, HEAD_DIM), F32)
    for src in range(n):
        weight = jnp.exp2(tops[src] - top)
        total = total + weight * (stats[src][:, 1:2] + stats[src][:, 2:3])
        num = num + weight * recv_buf[src, :unit, :].astype(F32)
    full = num / total
    for w in range(per_dev):
        c_row = w * requests
        f_row = per_dev * requests + w * requests
        out_ref[:, w * HEAD_DIM : (w + 1) * HEAD_DIM] = (
            gate_col[0][w] * full[c_row : c_row + requests]
            + gate_col[1][w] * full[f_row : f_row + requests]
        ).astype(BF16)
    for peer in peers:
        q_copy(me, peer).wait_send()
        p_copy(me, peer).wait_send()


def per_device(queries, gate_logits, kv_pool, page_table, selected, lengths):
    n = lax.axis_size("seq")
    slots, page_len, width = kv_pool.shape
    requests, cols = queries.shape
    if cols % HEAD_DIM != 0:
        return per_device_plain(queries, gate_logits, kv_pool, page_table, selected, lengths)
    per_dev = cols // HEAD_DIM
    unit = 2 * per_dev * requests
    dma = pltpu.SemaphoreType.DMA
    return pl.pallas_call(
        functools.partial(fused_kernel, n),
        out_shape=jax.ShapeDtypeStruct((requests, cols), BF16),
        in_specs=[pl.BlockSpec(memory_space=pltpu.HBM)] * 6,
        out_specs=pl.BlockSpec(memory_space=pltpu.VMEM),
        scratch_shapes=[
            pltpu.VMEM(kv_pool.shape, BF16),
            pltpu.VMEM((n, requests, cols), BF16),
            pltpu.VMEM(gate_logits.shape, F32),
            pltpu.VMEM(page_table.shape, jnp.int32),
            pltpu.VMEM(selected.shape, jnp.int32),
            pltpu.SMEM(lengths.shape, jnp.int32),
            pltpu.VMEM((per_dev, n * requests, HEAD_DIM), F32),
            pltpu.VMEM((n * 2 * unit, HEAD_DIM), F32),
            pltpu.VMEM((n, 2 * unit, HEAD_DIM), BF16),
            pltpu.VMEM((n, 2 * unit, HEAD_DIM), BF16),
            dma((slots // RUN,)),
            dma((5,)),
            dma((n,)),
            dma((n,)),
            dma((n,)),
            dma((n,)),
        ],
        compiler_params=pltpu.CompilerParams(
            collective_id=0, has_side_effects=True, vmem_limit_bytes=48 * 1024 * 1024
        ),
        name="paged_sparse_decode",
    )(queries, gate_logits, kv_pool, page_table, selected, lengths)


def solution(mesh):
    return jax.shard_map(
        per_device,
        mesh=mesh,
        in_specs=(
            P("grp", "seq"),
            P("grp", None),
            P(("grp", "seq"), None, None),
            P("grp", None),
            P("grp", None, None),
            P("grp"),
        ),
        out_specs=P("grp", "seq"),
        check_vma=False,
    )
```

```python
import functools
import math

import jax
import jax.numpy as jnp
from jax import lax
from jax.experimental import pallas as pl
from jax.experimental.pallas import tpu as pltpu
from jax.sharding import PartitionSpec as P

HEAD_DIM = 128


neg_big = -1e30


def joined(part, axis, combine):
    gathered = jax.tree.map(lambda a: lax.all_gather(a, axis), part)

    def take(source):
        return jax.tree.map(lambda a: lax.dynamic_index_in_dim(a, source, 0, False), gathered)

    return lax.fori_loop(
        1, lax.axis_size(axis), lambda source, state: combine(state, take(source)), take(0)
    )


def merge_pair(left, right):
    merged = ()
    for offset in (0, 3):
        row_top = jnp.maximum(left[offset], right[offset])
        left_scale = jnp.exp(left[offset] - row_top)
        right_scale = jnp.exp(right[offset] - row_top)
        merged = merged + (
            row_top,
            left[offset + 1] * left_scale + right[offset + 1] * right_scale,
            left[offset + 2] * left_scale[..., None] + right[offset + 2] * right_scale[..., None],
        )
    return merged


def per_device_plain(queries, gate_logits, kv_pool, page_table, selected, lengths):
    slot_count, page_len, double_width = kv_pool.shape
    kv_width = double_width // 2
    kv_heads = kv_width // HEAD_DIM
    requests = page_table.shape[0]
    ctx_pages = page_table.shape[1]
    col_count = queries.shape[1]
    highest = lax.Precision.HIGHEST
    all_queries = lax.all_gather(queries, "seq", axis=1, tiled=True)
    head_count = all_queries.shape[1] // HEAD_DIM
    group_size = head_count // kv_heads
    score_scale = 1.0 / math.sqrt(HEAD_DIM)
    first_slot = lax.axis_index("seq") * slot_count
    slot_ids = first_slot + jnp.arange(slot_count, dtype=jnp.int32)
    slot_match = page_table[:, :, None] == slot_ids[None, None, :]
    owner_hot = jnp.any(slot_match, axis=1)
    page_index = jnp.arange(ctx_pages, dtype=jnp.int32)
    page_of = jnp.sum(jnp.where(slot_match, page_index[None, :, None], 0), axis=(0, 1))
    slot_len = jnp.sum(jnp.where(owner_hot, lengths[:, None], 0), axis=0)
    owner_rows = jnp.dot(
        owner_hot.T.astype(jnp.bfloat16), all_queries, preferred_element_type=jnp.float32
    ).astype(jnp.bfloat16)
    slot_queries = owner_rows.reshape(slot_count, kv_heads, group_size, HEAD_DIM)
    key_rows = kv_pool[:, :, :kv_width].reshape(slot_count, page_len, kv_heads, HEAD_DIM)
    value_rows = kv_pool[:, :, kv_width:].reshape(slot_count, page_len, kv_heads, HEAD_DIM)
    position = page_of[:, None] * page_len + jnp.arange(page_len, dtype=jnp.int32)[None, :]
    is_valid = position < slot_len[:, None]
    is_live = page_of * page_len < slot_len
    valid_bf = is_valid.astype(jnp.bfloat16)
    counts = jnp.maximum(jnp.sum(is_valid.astype(jnp.float32), axis=1), 1.0)
    summary_keys = (
        jnp.einsum("st,stkd->skd", valid_bf, key_rows, preferred_element_type=jnp.float32)
        / counts[:, None, None]
    ).astype(jnp.bfloat16)
    summary_values = (
        jnp.einsum("st,stkd->skd", valid_bf, value_rows, preferred_element_type=jnp.float32)
        / counts[:, None, None]
    ).astype(jnp.bfloat16)
    coarse = (
        jnp.einsum("skgd,skd->skg", slot_queries, summary_keys, preferred_element_type=jnp.float32)
        * score_scale
    )
    coarse_mask = owner_hot[:, :, None, None] & is_live[None, :, None, None]
    coarse_masked = jnp.where(coarse_mask, coarse[None], neg_big)
    coarse_top = jnp.max(coarse_masked, axis=1)
    coarse_wt = jnp.where(coarse_mask, jnp.exp(coarse_masked - coarse_top[:, None]), 0.0)
    coarse_sum = jnp.sum(coarse_wt, axis=1)
    coarse_num = jnp.einsum(
        "rskg,skd->rkgd", coarse_wt, summary_values.astype(jnp.float32), precision=highest
    )
    fine_scores = (
        jnp.einsum("skgd,stkd->skgt", slot_queries, key_rows, preferred_element_type=jnp.float32)
        * score_scale
    )
    token_mask = is_valid[:, None, None, :]
    fine_masked = jnp.where(token_mask, fine_scores, neg_big)
    page_max = jnp.max(fine_masked, axis=3)
    page_wt = jnp.where(token_mask, jnp.exp(fine_masked - page_max[..., None]), 0.0).astype(
        jnp.bfloat16
    )
    page_sum = jnp.sum(page_wt.astype(jnp.float32), axis=3)
    page_num = jnp.einsum(
        "skgt,stkd->skgd", page_wt, value_rows, preferred_element_type=jnp.float32
    )
    page_hit = selected[:, None, :, :] == page_of[None, :, None, None]
    chosen = jnp.any(page_hit, axis=3) & owner_hot[:, :, None]
    chosen_full = chosen[..., None]
    sel_masked = jnp.where(chosen_full, page_max[None], neg_big)
    fine_top = jnp.max(sel_masked, axis=1)
    fine_wt = jnp.where(chosen_full, jnp.exp(sel_masked - fine_top[:, None]), 0.0)
    fine_sum = jnp.sum(fine_wt * page_sum[None], axis=1)
    fine_num = jnp.einsum("rskg,skgd->rkgd", fine_wt, page_num, precision=highest)
    gate_all = jax.nn.sigmoid(gate_logits)
    start_col = lax.axis_index("seq") * col_count
    coarse_gate = lax.dynamic_slice_in_dim(
        jnp.repeat(gate_all[:, :head_count], HEAD_DIM, axis=1), start_col, col_count, 1
    )
    fine_gate = lax.dynamic_slice_in_dim(
        jnp.repeat(gate_all[:, head_count:], HEAD_DIM, axis=1), start_col, col_count, 1
    )
    merged = joined(
        (coarse_top, coarse_sum, coarse_num, fine_top, fine_sum, fine_num), "seq", merge_pair
    )
    coarse_full = (merged[2] / merged[1][..., None]).reshape(requests, head_count * HEAD_DIM)
    fine_full = (merged[5] / merged[4][..., None]).reshape(requests, head_count * HEAD_DIM)
    coarse_cols = lax.dynamic_slice_in_dim(coarse_full, start_col, col_count, 1)
    fine_cols = lax.dynamic_slice_in_dim(fine_full, start_col, col_count, 1)
    return (coarse_gate * coarse_cols + fine_gate * fine_cols).astype(jnp.bfloat16)


RUN = 2
MESH = pl.DeviceIdType.MESH
F32 = jnp.float32
BF16 = jnp.bfloat16


def fused_kernel(
    n, q_hbm, gate_hbm, kv_hbm, pt_hbm, sel_hbm, len_hbm, out_ref,
    kv_buf, q_all, gate_v, pt_v, sel_v, len_s, q_even, gather_f, send_buf, recv_buf,
    kv_sem, in_sem, q_send, q_recv, p_send, p_recv,
):
    me = lax.axis_index("seq")
    slots, page_len, width = kv_buf.shape
    kv_width = width // 2
    kv_heads = kv_width // HEAD_DIM
    runs = slots // RUN
    span = RUN * page_len
    requests, ctx = pt_v.shape
    per_dev = q_all.shape[2] // HEAD_DIM
    heads = per_dev * n
    group = heads // kv_heads
    scale = math.log2(math.e) / math.sqrt(HEAD_DIM)

    def load_run(j):
        return pltpu.make_async_copy(
            kv_hbm.at[pl.ds(j * RUN, RUN)], kv_buf.at[pl.ds(j * RUN, RUN)], kv_sem.at[j]
        )

    small = [
        pltpu.make_async_copy(q_hbm, q_all.at[me], in_sem.at[0]),
        pltpu.make_async_copy(pt_hbm, pt_v, in_sem.at[1]),
        pltpu.make_async_copy(len_hbm, len_s, in_sem.at[2]),
        pltpu.make_async_copy(sel_hbm, sel_v, in_sem.at[3]),
        pltpu.make_async_copy(gate_hbm, gate_v, in_sem.at[4]),
    ]
    barrier = pltpu.get_barrier_semaphore()
    peers = [lax.rem(me + step, n) for step in range(1, n)]
    for peer in peers:
        pl.semaphore_signal(barrier, inc=1, device_id={"seq": peer}, device_id_type=MESH)
    for copy in small:
        copy.start()
    for j in range(runs):
        load_run(j).start()
    small[0].wait()
    pl.semaphore_wait(barrier, n - 1)

    def q_copy(slot, peer):
        return pltpu.make_async_remote_copy(
            src_ref=q_all.at[slot], dst_ref=q_all.at[slot], send_sem=q_send.at[peer],
            recv_sem=q_recv.at[slot], device_id={"seq": peer}, device_id_type=MESH,
        )

    for peer in peers:
        q_copy(me, peer).start()
    for copy in small[1:]:
        copy.wait()

    table = pt_v[...]
    row_id = lax.broadcasted_iota(jnp.int32, (requests, ctx), 0)
    col_f = lax.broadcasted_iota(jnp.int32, (requests, ctx), 1).astype(F32)
    len_grid = jnp.zeros((requests, ctx), F32)
    for r in range(requests):
        len_grid = jnp.where(row_id == r, len_s[r].astype(F32), len_grid)
    head_row = lax.broadcasted_iota(jnp.int32, (heads, 1), 0)
    head_id = lax.rem(head_row, n) * per_dev + head_row // n
    kv_row = head_id // group
    chosen_ids = []
    for r in range(requests):
        ids = sel_v[r].astype(F32)
        wide = jnp.zeros((heads, ids.shape[1]), F32)
        for k in range(kv_heads):
            wide = jnp.where(kv_row == k, ids[k : k + 1, :], wide)
        chosen_ids.append(wide)
    lane = lax.broadcasted_iota(jnp.int32, (1, span), 1)
    lane_f = lane.astype(F32)
    hot, valid, fine_ok, live, count = [], [], [], [], []
    for j in range(runs):
        match = table == me * slots + j * RUN
        page = jnp.sum(jnp.where(match, col_f, 0.0), axis=(0, 1), keepdims=True)
        length = jnp.sum(jnp.where(match, len_grid, 0.0), axis=(0, 1), keepdims=True)
        owner = jnp.max(jnp.where(match, 1.0, 0.0), axis=1, keepdims=True)
        hot_j = [owner[r : r + 1, :] for r in range(requests)]
        ids = chosen_ids[0] * hot_j[0]
        for r in range(1, requests):
            ids = ids + chosen_ids[r] * hot_j[r]
        valid_j = jnp.where(page * page_len + lane_f < length, 1.0, 0.0)
        ok = jnp.zeros((heads, span), F32)
        live_j, count_j = [], []
        for e in range(RUN):
            hit = jnp.max(jnp.where(ids == page + e, 1.0, 0.0), axis=1, keepdims=True)
            ok = jnp.where(lane // page_len == e, hit, ok)
            left = length - (page + e) * page_len
            live_j.append(jnp.where(left > 0.0, 1.0, 0.0))
            count_j.append(jnp.clip(left, 1.0, float(page_len)))
        hot.append(hot_j)
        valid.append(valid_j)
        fine_ok.append(ok * valid_j)
        live.append(live_j)
        count.append(count_j)

    for step, peer in enumerate(peers):
        q_copy(peer, peer).wait_recv()
    for src in range(n):
        rows = q_all[src].astype(F32)
        for w in range(per_dev):
            q_even[w, src * requests : (src + 1) * requests, :] = rows[
                :, w * HEAD_DIM : (w + 1) * HEAD_DIM
            ]
    q_rows = [
        jnp.concatenate(
            [q_even[w, pl.ds(r, n, stride=requests), :] for w in range(per_dev)], axis=0
        )
        for r in range(requests)
    ]

    fine_m, fine_l, fine_n, coarse_s, coarse_v = [], [], [], [], []
    valid_rows = 16
    row16 = lax.broadcasted_iota(jnp.int32, (valid_rows, span), 0)
    for j in range(runs):
        q_j = q_rows[0] * hot[j][0]
        for r in range(1, requests):
            q_j = q_j + q_rows[r] * hot[j][r]
        q_bd = jnp.concatenate(
            [jnp.where(kv_row == k, q_j, 0.0) for k in range(kv_heads)], axis=1
        ).astype(BF16)
        load_run(j).wait()
        keys = kv_buf[j * RUN : (j + 1) * RUN, :, :kv_width].reshape(span, kv_width)
        vals = kv_buf[j * RUN : (j + 1) * RUN, :, kv_width:].reshape(span, kv_width)
        scores = lax.dot_general(
            q_bd, keys, (((1,), (1,)), ((), ())), preferred_element_type=F32
        ) * scale
        ok = fine_ok[j] > 0.0
        masked = jnp.where(ok, scores, neg_big)
        top = jnp.max(masked, axis=1, keepdims=True)
        wt = jnp.where(ok, jnp.exp2(masked - top), 0.0).astype(BF16)
        fine_m.append(top)
        fine_l.append(jnp.sum(wt.astype(F32), axis=1, keepdims=True))
        shown = scores * valid[j]
        page_rows = jnp.where(lane // page_len == row16, valid[j], 0.0).astype(BF16)
        mixed = lax.dot_general(
            jnp.concatenate([wt, page_rows], axis=0), vals, (((1,), (0,)), ((), ())),
            preferred_element_type=F32,
        )
        num = mixed[:heads, :HEAD_DIM]
        for k in range(1, kv_heads):
            num = jnp.where(kv_row == k, mixed[:heads, k * HEAD_DIM : (k + 1) * HEAD_DIM], num)
        fine_n.append(num)
        for e in range(RUN):
            mean = jnp.sum(
                shown[:, e * page_len : (e + 1) * page_len], axis=1, keepdims=True
            ) / count[j][e]
            coarse_s.append(jnp.where(live[j][e] > 0.0, mean, neg_big))
            sv = (mixed[heads + e : heads + e + 1, :] / count[j][e]).astype(BF16).astype(F32)
            wide = jnp.broadcast_to(sv[:, :HEAD_DIM], (heads, HEAD_DIM))
            for k in range(1, kv_heads):
                wide = jnp.where(kv_row == k, sv[:, k * HEAD_DIM : (k + 1) * HEAD_DIM], wide)
            coarse_v.append(wide)

    unit = 2 * per_dev * requests
    lane_row = lax.broadcasted_iota(jnp.int32, (heads, HEAD_DIM), 1)

    def put(kind, r, top, total, num):
        top_b = top.astype(BF16).astype(F32)
        high = total.astype(BF16).astype(F32)
        stat = jnp.where(lane_row == 0, top_b, jnp.where(lane_row == 1, high, total - high))
        for w in range(per_dev):
            row = kind * per_dev * requests + w * requests + r
            gather_f[pl.ds(row, n, stride=2 * unit), :] = num[w * n : (w + 1) * n]
            gather_f[pl.ds(unit + row, n, stride=2 * unit), :] = stat[w * n : (w + 1) * n]

    for r in range(requests):
        for kind in range(2):
            if kind == 0:
                tops = coarse_s
                owner = [hot[i // RUN][r] for i in range(slots)]
            else:
                tops = fine_m
                owner = [hot[j][r] for j in range(runs)]
            held = [jnp.where(o > 0.0, t, neg_big) for o, t in zip(owner, tops)]
            top = functools.reduce(jnp.maximum, held)
            top = top.astype(BF16).astype(F32)
            total = jnp.zeros((heads, 1), F32)
            num = jnp.zeros((heads, HEAD_DIM), F32)
            for i, h in enumerate(held):
                weight = jnp.where(h > 0.5 * neg_big, jnp.exp2(h - top), 0.0)
                if kind == 0:
                    total = total + weight
                    num = num + weight * coarse_v[i]
                else:
                    total = total + weight * fine_l[i]
                    num = num + weight * fine_n[i]
            put(kind, r, top, total, num)
    for d in range(n):
        send_buf[d] = gather_f[d * 2 * unit : (d + 1) * 2 * unit, :].astype(BF16)

    def p_copy(slot, peer):
        return pltpu.make_async_remote_copy(
            src_ref=send_buf.at[peer], dst_ref=recv_buf.at[slot], send_sem=p_send.at[peer],
            recv_sem=p_recv.at[slot], device_id={"seq": peer}, device_id_type=MESH,
        )

    for peer in peers:
        p_copy(me, peer).start()
    recv_buf[me] = send_buf[me]
    gates = jax.nn.sigmoid(gate_v[...])
    gate_lane = lax.broadcasted_iota(jnp.int32, gates.shape, 1)
    gate_col = [
        [
            jnp.sum(
                jnp.where(gate_lane == kind * heads + me * per_dev + w, gates, 0.0),
                axis=1, keepdims=True,
            )
            for w in range(per_dev)
        ]
        for kind in range(2)
    ]
    for peer in peers:
        p_copy(peer, peer).wait_recv()
    stats = [recv_buf[src, unit:, :].astype(F32) for src in range(n)]
    tops = [s[:, 0:1] for s in stats]
    top = functools.reduce(jnp.maximum, tops)
    total = jnp.zeros((unit, 1), F32)
    num = jnp.zeros((unit, HEAD_DIM), F32)
    for src in range(n):
        weight = jnp.exp2(tops[src] - top)
        total = total + weight * (stats[src][:, 1:2] + stats[src][:, 2:3])
        num = num + weight * recv_buf[src, :unit, :].astype(F32)
    full = num / total
    for w in range(per_dev):
        c_row = w * requests
        f_row = per_dev * requests + w * requests
        out_ref[:, w * HEAD_DIM : (w + 1) * HEAD_DIM] = (
            gate_col[0][w] * full[c_row : c_row + requests]
            + gate_col[1][w] * full[f_row : f_row + requests]
        ).astype(BF16)
    for peer in peers:
        q_copy(me, peer).wait_send()
        p_copy(me, peer).wait_send()


def per_device(queries, gate_logits, kv_pool, page_table, selected, lengths):
    n = lax.axis_size("seq")
    slots, page_len, width = kv_pool.shape
    requests, cols = queries.shape
    if cols % HEAD_DIM != 0:
        return per_device_plain(queries, gate_logits, kv_pool, page_table, selected, lengths)
    per_dev = cols // HEAD_DIM
    unit = 2 * per_dev * requests
    dma = pltpu.SemaphoreType.DMA
    return pl.pallas_call(
        functools.partial(fused_kernel, n),
        out_shape=jax.ShapeDtypeStruct((requests, cols), BF16),
        in_specs=[pl.BlockSpec(memory_space=pltpu.HBM)] * 6,
        out_specs=pl.BlockSpec(memory_space=pltpu.VMEM),
        scratch_shapes=[
            pltpu.VMEM(kv_pool.shape, BF16),
            pltpu.VMEM((n, requests, cols), BF16),
            pltpu.VMEM(gate_logits.shape, F32),
            pltpu.VMEM(page_table.shape, jnp.int32),
            pltpu.VMEM(selected.shape, jnp.int32),
            pltpu.SMEM(lengths.shape, jnp.int32),
            pltpu.VMEM((per_dev, n * requests, HEAD_DIM), F32),
            pltpu.VMEM((n * 2 * unit, HEAD_DIM), F32),
            pltpu.VMEM((n, 2 * unit, HEAD_DIM), BF16),
            pltpu.VMEM((n, 2 * unit, HEAD_DIM), BF16),
            dma((slots // RUN,)),
            dma((5,)),
            dma((n,)),
            dma((n,)),
            dma((n,)),
            dma((n,)),
        ],
        compiler_params=pltpu.CompilerParams(
            collective_id=0, has_side_effects=True, vmem_limit_bytes=67043328
        ),
        name="paged_sparse_decode",
    )(queries, gate_logits, kv_pool, page_table, selected, lengths)


def solution(mesh):
    return jax.shard_map(
        per_device,
        mesh=mesh,
        in_specs=(
            P("grp", "seq"),
            P("grp", None),
            P(("grp", "seq"), None, None),
            P("grp", None),
            P("grp", None, None),
            P("grp"),
        ),
        out_specs=P("grp", "seq"),
        check_vma=False,
    )
```

```python
import functools
import math

import jax
import jax.numpy as jnp
from jax import lax
from jax.experimental import pallas as pl
from jax.experimental.pallas import tpu as pltpu
from jax.sharding import PartitionSpec as P

HEAD_DIM = 128


neg_big = -1e30


def joined(part, axis, combine):
    gathered = jax.tree.map(lambda a: lax.all_gather(a, axis), part)

    def take(source):
        return jax.tree.map(lambda a: lax.dynamic_index_in_dim(a, source, 0, False), gathered)

    return lax.fori_loop(
        1, lax.axis_size(axis), lambda source, state: combine(state, take(source)), take(0)
    )


def merge_pair(left, right):
    merged = ()
    for offset in (0, 3):
        row_top = jnp.maximum(left[offset], right[offset])
        left_scale = jnp.exp(left[offset] - row_top)
        right_scale = jnp.exp(right[offset] - row_top)
        merged = merged + (
            row_top,
            left[offset + 1] * left_scale + right[offset + 1] * right_scale,
            left[offset + 2] * left_scale[..., None] + right[offset + 2] * right_scale[..., None],
        )
    return merged


def per_device_plain(queries, gate_logits, kv_pool, page_table, selected, lengths):
    slot_count, page_len, double_width = kv_pool.shape
    kv_width = double_width // 2
    kv_heads = kv_width // HEAD_DIM
    requests = page_table.shape[0]
    ctx_pages = page_table.shape[1]
    col_count = queries.shape[1]
    highest = lax.Precision.HIGHEST
    all_queries = lax.all_gather(queries, "seq", axis=1, tiled=True)
    head_count = all_queries.shape[1] // HEAD_DIM
    group_size = head_count // kv_heads
    score_scale = 1.0 / math.sqrt(HEAD_DIM)
    first_slot = lax.axis_index("seq") * slot_count
    slot_ids = first_slot + jnp.arange(slot_count, dtype=jnp.int32)
    slot_match = page_table[:, :, None] == slot_ids[None, None, :]
    owner_hot = jnp.any(slot_match, axis=1)
    page_index = jnp.arange(ctx_pages, dtype=jnp.int32)
    page_of = jnp.sum(jnp.where(slot_match, page_index[None, :, None], 0), axis=(0, 1))
    slot_len = jnp.sum(jnp.where(owner_hot, lengths[:, None], 0), axis=0)
    owner_rows = jnp.dot(
        owner_hot.T.astype(jnp.bfloat16), all_queries, preferred_element_type=jnp.float32
    ).astype(jnp.bfloat16)
    slot_queries = owner_rows.reshape(slot_count, kv_heads, group_size, HEAD_DIM)
    key_rows = kv_pool[:, :, :kv_width].reshape(slot_count, page_len, kv_heads, HEAD_DIM)
    value_rows = kv_pool[:, :, kv_width:].reshape(slot_count, page_len, kv_heads, HEAD_DIM)
    position = page_of[:, None] * page_len + jnp.arange(page_len, dtype=jnp.int32)[None, :]
    is_valid = position < slot_len[:, None]
    is_live = page_of * page_len < slot_len
    valid_bf = is_valid.astype(jnp.bfloat16)
    counts = jnp.maximum(jnp.sum(is_valid.astype(jnp.float32), axis=1), 1.0)
    summary_keys = (
        jnp.einsum("st,stkd->skd", valid_bf, key_rows, preferred_element_type=jnp.float32)
        / counts[:, None, None]
    ).astype(jnp.bfloat16)
    summary_values = (
        jnp.einsum("st,stkd->skd", valid_bf, value_rows, preferred_element_type=jnp.float32)
        / counts[:, None, None]
    ).astype(jnp.bfloat16)
    coarse = (
        jnp.einsum("skgd,skd->skg", slot_queries, summary_keys, preferred_element_type=jnp.float32)
        * score_scale
    )
    coarse_mask = owner_hot[:, :, None, None] & is_live[None, :, None, None]
    coarse_masked = jnp.where(coarse_mask, coarse[None], neg_big)
    coarse_top = jnp.max(coarse_masked, axis=1)
    coarse_wt = jnp.where(coarse_mask, jnp.exp(coarse_masked - coarse_top[:, None]), 0.0)
    coarse_sum = jnp.sum(coarse_wt, axis=1)
    coarse_num = jnp.einsum(
        "rskg,skd->rkgd", coarse_wt, summary_values.astype(jnp.float32), precision=highest
    )
    fine_scores = (
        jnp.einsum("skgd,stkd->skgt", slot_queries, key_rows, preferred_element_type=jnp.float32)
        * score_scale
    )
    token_mask = is_valid[:, None, None, :]
    fine_masked = jnp.where(token_mask, fine_scores, neg_big)
    page_max = jnp.max(fine_masked, axis=3)
    page_wt = jnp.where(token_mask, jnp.exp(fine_masked - page_max[..., None]), 0.0).astype(
        jnp.bfloat16
    )
    page_sum = jnp.sum(page_wt.astype(jnp.float32), axis=3)
    page_num = jnp.einsum(
        "skgt,stkd->skgd", page_wt, value_rows, preferred_element_type=jnp.float32
    )
    page_hit = selected[:, None, :, :] == page_of[None, :, None, None]
    chosen = jnp.any(page_hit, axis=3) & owner_hot[:, :, None]
    chosen_full = chosen[..., None]
    sel_masked = jnp.where(chosen_full, page_max[None], neg_big)
    fine_top = jnp.max(sel_masked, axis=1)
    fine_wt = jnp.where(chosen_full, jnp.exp(sel_masked - fine_top[:, None]), 0.0)
    fine_sum = jnp.sum(fine_wt * page_sum[None], axis=1)
    fine_num = jnp.einsum("rskg,skgd->rkgd", fine_wt, page_num, precision=highest)
    gate_all = jax.nn.sigmoid(gate_logits)
    start_col = lax.axis_index("seq") * col_count
    coarse_gate = lax.dynamic_slice_in_dim(
        jnp.repeat(gate_all[:, :head_count], HEAD_DIM, axis=1), start_col, col_count, 1
    )
    fine_gate = lax.dynamic_slice_in_dim(
        jnp.repeat(gate_all[:, head_count:], HEAD_DIM, axis=1), start_col, col_count, 1
    )
    merged = joined(
        (coarse_top, coarse_sum, coarse_num, fine_top, fine_sum, fine_num), "seq", merge_pair
    )
    coarse_full = (merged[2] / merged[1][..., None]).reshape(requests, head_count * HEAD_DIM)
    fine_full = (merged[5] / merged[4][..., None]).reshape(requests, head_count * HEAD_DIM)
    coarse_cols = lax.dynamic_slice_in_dim(coarse_full, start_col, col_count, 1)
    fine_cols = lax.dynamic_slice_in_dim(fine_full, start_col, col_count, 1)
    return (coarse_gate * coarse_cols + fine_gate * fine_cols).astype(jnp.bfloat16)


RUN = 2
MESH = pl.DeviceIdType.MESH
F32 = jnp.float32
BF16 = jnp.bfloat16


def fused_kernel(
    n, q_hbm, gate_hbm, kv_hbm, pt_hbm, sel_hbm, len_hbm, out_ref,
    kv_buf, q_all, gate_v, pt_v, sel_v, len_s, q_even, sum_k, sum_v, gather_f, send_buf, recv_buf,
    kv_sem, in_sem, q_send, q_recv, p_send, p_recv,
):
    me = lax.axis_index("seq")
    slots, page_len, width = kv_buf.shape
    kv_width = width // 2
    kv_heads = kv_width // HEAD_DIM
    runs = slots // RUN
    span = RUN * page_len
    requests, ctx = pt_v.shape
    per_dev = q_all.shape[2] // HEAD_DIM
    heads = per_dev * n
    group = heads // kv_heads
    scale = math.log2(math.e) / math.sqrt(HEAD_DIM)

    def load_run(j):
        return pltpu.make_async_copy(
            kv_hbm.at[pl.ds(j * RUN, RUN)], kv_buf.at[pl.ds(j * RUN, RUN)], kv_sem.at[j]
        )

    small = [
        pltpu.make_async_copy(q_hbm, q_all.at[me], in_sem.at[0]),
        pltpu.make_async_copy(pt_hbm, pt_v, in_sem.at[1]),
        pltpu.make_async_copy(len_hbm, len_s, in_sem.at[2]),
        pltpu.make_async_copy(sel_hbm, sel_v, in_sem.at[3]),
        pltpu.make_async_copy(gate_hbm, gate_v, in_sem.at[4]),
    ]
    barrier = pltpu.get_barrier_semaphore()
    peers = [lax.rem(me + step, n) for step in range(1, n)]
    for peer in peers:
        pl.semaphore_signal(barrier, inc=1, device_id={"seq": peer}, device_id_type=MESH)
    for copy in small:
        copy.start()
    for j in range(runs):
        load_run(j).start()
    small[0].wait()
    pl.semaphore_wait(barrier, n - 1)

    def q_copy(slot, peer):
        return pltpu.make_async_remote_copy(
            src_ref=q_all.at[slot], dst_ref=q_all.at[slot], send_sem=q_send.at[peer],
            recv_sem=q_recv.at[slot], device_id={"seq": peer}, device_id_type=MESH,
        )

    for peer in peers:
        q_copy(me, peer).start()
    for copy in small[1:]:
        copy.wait()

    table = pt_v[...]
    row_id = lax.broadcasted_iota(jnp.int32, (requests, ctx), 0)
    col_f = lax.broadcasted_iota(jnp.int32, (requests, ctx), 1).astype(F32)
    len_grid = jnp.zeros((requests, ctx), F32)
    for r in range(requests):
        len_grid = jnp.where(row_id == r, len_s[r].astype(F32), len_grid)
    head_row = lax.broadcasted_iota(jnp.int32, (heads, 1), 0)
    head_id = lax.rem(head_row, n) * per_dev + head_row // n
    kv_row = head_id // group
    chosen_ids = []
    for r in range(requests):
        ids = sel_v[r].astype(F32)
        wide = jnp.zeros((heads, ids.shape[1]), F32)
        for k in range(kv_heads):
            wide = jnp.where(kv_row == k, ids[k : k + 1, :], wide)
        chosen_ids.append(wide)
    lane = lax.broadcasted_iota(jnp.int32, (1, span), 1)
    lane_f = lane.astype(F32)
    hot, valid, fine_ok, live, count = [], [], [], [], []
    for j in range(runs):
        match = table == me * slots + j * RUN
        page = jnp.sum(jnp.where(match, col_f, 0.0), axis=(0, 1), keepdims=True)
        length = jnp.sum(jnp.where(match, len_grid, 0.0), axis=(0, 1), keepdims=True)
        owner = jnp.max(jnp.where(match, 1.0, 0.0), axis=1, keepdims=True)
        hot_j = [owner[r : r + 1, :] for r in range(requests)]
        ids = chosen_ids[0] * hot_j[0]
        for r in range(1, requests):
            ids = ids + chosen_ids[r] * hot_j[r]
        valid_j = jnp.where(page * page_len + lane_f < length, 1.0, 0.0)
        ok = jnp.zeros((heads, span), F32)
        live_j, count_j = [], []
        for e in range(RUN):
            hit = jnp.max(jnp.where(ids == page + e, 1.0, 0.0), axis=1, keepdims=True)
            ok = jnp.where(lane // page_len == e, hit, ok)
            left = length - (page + e) * page_len
            live_j.append(jnp.where(left > 0.0, 1.0, 0.0))
            count_j.append(jnp.clip(left, 1.0, float(page_len)))
        hot.append(hot_j)
        valid.append(valid_j)
        fine_ok.append(ok * valid_j)
        live.append(live_j)
        count.append(count_j)

    row16 = lax.broadcasted_iota(jnp.int32, (16, span), 0)

    def by_head(row):
        wide = jnp.broadcast_to(row[:, :HEAD_DIM], (heads, HEAD_DIM))
        for k in range(1, kv_heads):
            wide = jnp.where(kv_row == k, row[:, k * HEAD_DIM : (k + 1) * HEAD_DIM], wide)
        return wide

    for j in range(runs):
        load_run(j).wait()
        page_rows = jnp.where(lane // page_len == row16, valid[j], 0.0).astype(BF16)
        sums = jnp.dot(
            page_rows, kv_buf[j * RUN : (j + 1) * RUN].reshape(span, width),
            preferred_element_type=F32,
        )
        for e in range(RUN):
            mean = (sums[e : e + 1, :] / count[j][e]).astype(BF16).astype(F32)
            sum_k[j * RUN + e] = by_head(mean[:, :kv_width])
            sum_v[j * RUN + e] = by_head(mean[:, kv_width:])

    for step, peer in enumerate(peers):
        q_copy(peer, peer).wait_recv()
    for src in range(n):
        rows = q_all[src].astype(F32)
        for w in range(per_dev):
            q_even[w, src * requests : (src + 1) * requests, :] = rows[
                :, w * HEAD_DIM : (w + 1) * HEAD_DIM
            ]
    q_rows = [
        jnp.concatenate(
            [q_even[w, pl.ds(r, n, stride=requests), :] for w in range(per_dev)], axis=0
        )
        for r in range(requests)
    ]
    kv_col = jnp.broadcast_to(kv_row, (heads, HEAD_DIM))
    own = [jnp.where(kv_col == k, 1.0, 0.0).astype(BF16) for k in range(kv_heads)]

    scores, coarse_s = [], []
    for j in range(runs):
        q_j = q_rows[0] * hot[j][0]
        for r in range(1, requests):
            q_j = q_j + q_rows[r] * hot[j][r]
        q_b = q_j.astype(BF16)
        q_bd = jnp.concatenate([q_b * own[k] for k in range(kv_heads)], axis=1)
        keys = kv_buf[j * RUN : (j + 1) * RUN, :, :kv_width].reshape(span, kv_width)
        scores.append(
            lax.dot_general(
                q_bd, keys, (((1,), (1,)), ((), ())), preferred_element_type=F32
            )
        )
        pair = []
        for e in range(RUN):
            dot = jnp.sum(q_j * sum_k[j * RUN + e], axis=1, keepdims=True) * scale
            pair.append(jnp.where(live[j][e] > 0.0, dot, neg_big))
        coarse_s.append(pair)
    fine_m, fine_l, weights = [], [], []
    for j in range(runs):
        ok = fine_ok[j] > 0.0
        masked = jnp.where(ok, scores[j] * scale, neg_big)
        top = jnp.max(masked, axis=1, keepdims=True)
        wt = jnp.where(ok, jnp.exp2(masked - top), 0.0).astype(BF16)
        fine_m.append(top)
        fine_l.append(jnp.sum(wt.astype(F32), axis=1, keepdims=True))
        weights.append(wt)
    fine_n = []
    for j in range(runs):
        vals = kv_buf[j * RUN : (j + 1) * RUN, :, kv_width:].reshape(span, kv_width)
        mixed = jnp.dot(weights[j], vals, preferred_element_type=F32)
        num = mixed[:, :HEAD_DIM]
        for k in range(1, kv_heads):
            num = jnp.where(kv_row == k, mixed[:, k * HEAD_DIM : (k + 1) * HEAD_DIM], num)
        fine_n.append(num)

    kind_rows = per_dev * requests
    unit = 2 * kind_rows
    rows_out = unit + kind_rows
    lane_id = lax.broadcasted_iota(jnp.int32, (heads, HEAD_DIM), 1)

    def request_tops(run_tops):
        tops = []
        for r in range(requests):
            held = [jnp.where(hot[j][r] > 0.0, run_tops[j], neg_big) for j in range(runs)]
            tops.append(functools.reduce(jnp.maximum, held).astype(BF16).astype(F32))
        return tops

    def of_run(tops, j):
        mine = tops[0] * hot[j][0]
        for r in range(1, requests):
            mine = mine + tops[r] * hot[j][r]
        return mine

    def weight_of(score, base):
        return jnp.where(score > 0.5 * neg_big, jnp.exp2(score - base), 0.0)

    def split_by_request(parts):
        totals = []
        for r in range(requests):
            total = parts[0] * hot[0][r]
            for j in range(1, runs):
                total = total + parts[j] * hot[j][r]
            totals.append(total)
        return totals

    coarse_tops = request_tops([functools.reduce(jnp.maximum, pair) for pair in coarse_s])
    coarse_sum, coarse_num = [], []
    for j in range(runs):
        base = of_run(coarse_tops, j)
        wts = [weight_of(s, base) for s in coarse_s[j]]
        coarse_sum.append(functools.reduce(jnp.add, wts))
        coarse_num.append(
            functools.reduce(jnp.add, [wts[e] * sum_v[j * RUN + e] for e in range(RUN)])
        )
    fine_tops = request_tops(fine_m)
    fine_sum, fine_num = [], []
    for j in range(runs):
        wt = weight_of(fine_m[j], of_run(fine_tops, j))
        fine_sum.append(wt * fine_l[j])
        fine_num.append(wt * fine_n[j])
    tops = [coarse_tops, fine_tops]
    sums = [split_by_request(coarse_sum), split_by_request(fine_sum)]
    nums = [split_by_request(coarse_num), split_by_request(fine_num)]
    for r in range(requests):
        stat = jnp.zeros((heads, HEAD_DIM), F32)
        for kind in range(2):
            high = sums[kind][r].astype(BF16).astype(F32)
            for i, value in enumerate((tops[kind][r], high, sums[kind][r] - high)):
                stat = jnp.where(lane_id == 3 * kind + i, value, stat)
        for w in range(per_dev):
            part = slice(w * n, (w + 1) * n)
            row = w * requests + r
            for kind in range(2):
                gather_f[pl.ds(kind * kind_rows + row, n, stride=rows_out), :] = nums[kind][r][part]
            gather_f[pl.ds(unit + row, n, stride=rows_out), :] = stat[part]
    for d in range(n):
        send_buf[d] = gather_f[d * rows_out : (d + 1) * rows_out, :].astype(BF16)

    def p_copy(slot, peer):
        return pltpu.make_async_remote_copy(
            src_ref=send_buf.at[peer], dst_ref=recv_buf.at[slot], send_sem=p_send.at[peer],
            recv_sem=p_recv.at[slot], device_id={"seq": peer}, device_id_type=MESH,
        )

    for peer in peers:
        p_copy(me, peer).start()
    recv_buf[me] = send_buf[me]
    gates = jax.nn.sigmoid(gate_v[...])
    gate_lane = lax.broadcasted_iota(jnp.int32, gates.shape, 1)
    gate_col = [
        [
            jnp.sum(
                jnp.where(gate_lane == kind * heads + me * per_dev + w, gates, 0.0),
                axis=1, keepdims=True,
            )
            for w in range(per_dev)
        ]
        for kind in range(2)
    ]
    for peer in peers:
        p_copy(peer, peer).wait_recv()
    stats = [recv_buf[src, unit:, :].astype(F32) for src in range(n)]
    full = []
    for kind in range(2):
        tops = [s[:, 3 * kind : 3 * kind + 1] for s in stats]
        top = functools.reduce(jnp.maximum, tops)
        total = jnp.zeros((kind_rows, 1), F32)
        num = jnp.zeros((kind_rows, HEAD_DIM), F32)
        part = slice(kind * kind_rows, (kind + 1) * kind_rows)
        for src in range(n):
            weight = jnp.exp2(tops[src] - top)
            both = stats[src][:, 3 * kind + 1 : 3 * kind + 2] + stats[src][:, 3 * kind + 2 : 3 * kind + 3]
            total = total + weight * both
            num = num + weight * recv_buf[src, part, :].astype(F32)
        full.append(num / total)
    for w in range(per_dev):
        part = slice(w * requests, (w + 1) * requests)
        out_ref[:, w * HEAD_DIM : (w + 1) * HEAD_DIM] = (
            gate_col[0][w] * full[0][part] + gate_col[1][w] * full[1][part]
        ).astype(BF16)
    for peer in peers:
        q_copy(me, peer).wait_send()
        p_copy(me, peer).wait_send()


def per_device(queries, gate_logits, kv_pool, page_table, selected, lengths):
    n = lax.axis_size("seq")
    slots, page_len, width = kv_pool.shape
    requests, cols = queries.shape
    if cols % HEAD_DIM != 0:
        return per_device_plain(queries, gate_logits, kv_pool, page_table, selected, lengths)
    per_dev = cols // HEAD_DIM
    rows_out = 3 * per_dev * requests
    dma = pltpu.SemaphoreType.DMA
    return pl.pallas_call(
        functools.partial(fused_kernel, n),
        out_shape=jax.ShapeDtypeStruct((requests, cols), BF16),
        in_specs=[pl.BlockSpec(memory_space=pltpu.HBM)] * 6,
        out_specs=pl.BlockSpec(memory_space=pltpu.VMEM),
        scratch_shapes=[
            pltpu.VMEM(kv_pool.shape, BF16),
            pltpu.VMEM((n, requests, cols), BF16),
            pltpu.VMEM(gate_logits.shape, F32),
            pltpu.VMEM(page_table.shape, jnp.int32),
            pltpu.VMEM(selected.shape, jnp.int32),
            pltpu.SMEM(lengths.shape, jnp.int32),
            pltpu.VMEM((per_dev, n * requests, HEAD_DIM), F32),
            pltpu.VMEM((slots, per_dev * n, HEAD_DIM), F32),
            pltpu.VMEM((slots, per_dev * n, HEAD_DIM), F32),
            pltpu.VMEM((n * rows_out, HEAD_DIM), F32),
            pltpu.VMEM((n, rows_out, HEAD_DIM), BF16),
            pltpu.VMEM((n, rows_out, HEAD_DIM), BF16),
            dma((slots // RUN,)),
            dma((5,)),
            dma((n,)),
            dma((n,)),
            dma((n,)),
            dma((n,)),
        ],
        compiler_params=pltpu.CompilerParams(
            collective_id=0, has_side_effects=True, vmem_limit_bytes=67043328
        ),
        name="paged_sparse_decode",
    )(queries, gate_logits, kv_pool, page_table, selected, lengths)


def solution(mesh):
    return jax.shard_map(
        per_device,
        mesh=mesh,
        in_specs=(
            P("grp", "seq"),
            P("grp", None),
            P(("grp", "seq"), None, None),
            P("grp", None),
            P("grp", None, None),
            P("grp"),
        ),
        out_specs=P("grp", "seq"),
        check_vma=False,
    )
```

```python
import functools
import math

import jax
import jax.numpy as jnp
from jax import lax
from jax.experimental import pallas as pl
from jax.experimental.pallas import tpu as pltpu
from jax.sharding import PartitionSpec as P

HEAD_DIM = 128


neg_big = -1e30


def joined(part, axis, combine):
    gathered = jax.tree.map(lambda a: lax.all_gather(a, axis), part)

    def take(source):
        return jax.tree.map(lambda a: lax.dynamic_index_in_dim(a, source, 0, False), gathered)

    return lax.fori_loop(
        1, lax.axis_size(axis), lambda source, state: combine(state, take(source)), take(0)
    )


def merge_pair(left, right):
    merged = ()
    for offset in (0, 3):
        row_top = jnp.maximum(left[offset], right[offset])
        left_scale = jnp.exp(left[offset] - row_top)
        right_scale = jnp.exp(right[offset] - row_top)
        merged = merged + (
            row_top,
            left[offset + 1] * left_scale + right[offset + 1] * right_scale,
            left[offset + 2] * left_scale[..., None] + right[offset + 2] * right_scale[..., None],
        )
    return merged


def per_device_plain(queries, gate_logits, kv_pool, page_table, selected, lengths):
    slot_count, page_len, double_width = kv_pool.shape
    kv_width = double_width // 2
    kv_heads = kv_width // HEAD_DIM
    requests = page_table.shape[0]
    ctx_pages = page_table.shape[1]
    col_count = queries.shape[1]
    highest = lax.Precision.HIGHEST
    all_queries = lax.all_gather(queries, "seq", axis=1, tiled=True)
    head_count = all_queries.shape[1] // HEAD_DIM
    group_size = head_count // kv_heads
    score_scale = 1.0 / math.sqrt(HEAD_DIM)
    first_slot = lax.axis_index("seq") * slot_count
    slot_ids = first_slot + jnp.arange(slot_count, dtype=jnp.int32)
    slot_match = page_table[:, :, None] == slot_ids[None, None, :]
    owner_hot = jnp.any(slot_match, axis=1)
    page_index = jnp.arange(ctx_pages, dtype=jnp.int32)
    page_of = jnp.sum(jnp.where(slot_match, page_index[None, :, None], 0), axis=(0, 1))
    slot_len = jnp.sum(jnp.where(owner_hot, lengths[:, None], 0), axis=0)
    owner_rows = jnp.dot(
        owner_hot.T.astype(jnp.bfloat16), all_queries, preferred_element_type=jnp.float32
    ).astype(jnp.bfloat16)
    slot_queries = owner_rows.reshape(slot_count, kv_heads, group_size, HEAD_DIM)
    key_rows = kv_pool[:, :, :kv_width].reshape(slot_count, page_len, kv_heads, HEAD_DIM)
    value_rows = kv_pool[:, :, kv_width:].reshape(slot_count, page_len, kv_heads, HEAD_DIM)
    position = page_of[:, None] * page_len + jnp.arange(page_len, dtype=jnp.int32)[None, :]
    is_valid = position < slot_len[:, None]
    is_live = page_of * page_len < slot_len
    valid_bf = is_valid.astype(jnp.bfloat16)
    counts = jnp.maximum(jnp.sum(is_valid.astype(jnp.float32), axis=1), 1.0)
    summary_keys = (
        jnp.einsum("st,stkd->skd", valid_bf, key_rows, preferred_element_type=jnp.float32)
        / counts[:, None, None]
    ).astype(jnp.bfloat16)
    summary_values = (
        jnp.einsum("st,stkd->skd", valid_bf, value_rows, preferred_element_type=jnp.float32)
        / counts[:, None, None]
    ).astype(jnp.bfloat16)
    coarse = (
        jnp.einsum("skgd,skd->skg", slot_queries, summary_keys, preferred_element_type=jnp.float32)
        * score_scale
    )
    coarse_mask = owner_hot[:, :, None, None] & is_live[None, :, None, None]
    coarse_masked = jnp.where(coarse_mask, coarse[None], neg_big)
    coarse_top = jnp.max(coarse_masked, axis=1)
    coarse_wt = jnp.where(coarse_mask, jnp.exp(coarse_masked - coarse_top[:, None]), 0.0)
    coarse_sum = jnp.sum(coarse_wt, axis=1)
    coarse_num = jnp.einsum(
        "rskg,skd->rkgd", coarse_wt, summary_values.astype(jnp.float32), precision=highest
    )
    fine_scores = (
        jnp.einsum("skgd,stkd->skgt", slot_queries, key_rows, preferred_element_type=jnp.float32)
        * score_scale
    )
    token_mask = is_valid[:, None, None, :]
    fine_masked = jnp.where(token_mask, fine_scores, neg_big)
    page_max = jnp.max(fine_masked, axis=3)
    page_wt = jnp.where(token_mask, jnp.exp(fine_masked - page_max[..., None]), 0.0).astype(
        jnp.bfloat16
    )
    page_sum = jnp.sum(page_wt.astype(jnp.float32), axis=3)
    page_num = jnp.einsum(
        "skgt,stkd->skgd", page_wt, value_rows, preferred_element_type=jnp.float32
    )
    page_hit = selected[:, None, :, :] == page_of[None, :, None, None]
    chosen = jnp.any(page_hit, axis=3) & owner_hot[:, :, None]
    chosen_full = chosen[..., None]
    sel_masked = jnp.where(chosen_full, page_max[None], neg_big)
    fine_top = jnp.max(sel_masked, axis=1)
    fine_wt = jnp.where(chosen_full, jnp.exp(sel_masked - fine_top[:, None]), 0.0)
    fine_sum = jnp.sum(fine_wt * page_sum[None], axis=1)
    fine_num = jnp.einsum("rskg,skgd->rkgd", fine_wt, page_num, precision=highest)
    gate_all = jax.nn.sigmoid(gate_logits)
    start_col = lax.axis_index("seq") * col_count
    coarse_gate = lax.dynamic_slice_in_dim(
        jnp.repeat(gate_all[:, :head_count], HEAD_DIM, axis=1), start_col, col_count, 1
    )
    fine_gate = lax.dynamic_slice_in_dim(
        jnp.repeat(gate_all[:, head_count:], HEAD_DIM, axis=1), start_col, col_count, 1
    )
    merged = joined(
        (coarse_top, coarse_sum, coarse_num, fine_top, fine_sum, fine_num), "seq", merge_pair
    )
    coarse_full = (merged[2] / merged[1][..., None]).reshape(requests, head_count * HEAD_DIM)
    fine_full = (merged[5] / merged[4][..., None]).reshape(requests, head_count * HEAD_DIM)
    coarse_cols = lax.dynamic_slice_in_dim(coarse_full, start_col, col_count, 1)
    fine_cols = lax.dynamic_slice_in_dim(fine_full, start_col, col_count, 1)
    return (coarse_gate * coarse_cols + fine_gate * fine_cols).astype(jnp.bfloat16)


RUN = 2
MESH = pl.DeviceIdType.MESH
F32 = jnp.float32
BF16 = jnp.bfloat16


def fused_kernel(
    n, q_hbm, gate_hbm, kv_hbm, pt_hbm, sel_hbm, len_hbm, out_ref,
    kv_buf, q_all, gate_v, pt_v, sel_v, len_s, q_even, sum_k, sum_v, gather_f, send_buf, recv_buf,
    kv_sem, in_sem, q_send, q_recv, p_send, p_recv,
):
    me = lax.axis_index("seq")
    slots, page_len, width = kv_buf.shape
    kv_width = width // 2
    kv_heads = kv_width // HEAD_DIM
    runs = slots // RUN
    span = RUN * page_len
    requests, ctx = pt_v.shape
    per_dev = q_all.shape[2] // HEAD_DIM
    heads = per_dev * n
    group = heads // kv_heads
    scale = math.log2(math.e) / math.sqrt(HEAD_DIM)

    def load_run(j):
        return pltpu.make_async_copy(
            kv_hbm.at[pl.ds(j * RUN, RUN)], kv_buf.at[pl.ds(j * RUN, RUN)], kv_sem.at[j]
        )

    small = [
        pltpu.make_async_copy(q_hbm, q_all.at[me], in_sem.at[0]),
        pltpu.make_async_copy(pt_hbm, pt_v, in_sem.at[1]),
        pltpu.make_async_copy(len_hbm, len_s, in_sem.at[2]),
        pltpu.make_async_copy(sel_hbm, sel_v, in_sem.at[3]),
        pltpu.make_async_copy(gate_hbm, gate_v, in_sem.at[4]),
    ]
    barrier = pltpu.get_barrier_semaphore()
    peers = [lax.rem(me + step, n) for step in range(1, n)]
    for peer in peers:
        pl.semaphore_signal(barrier, inc=1, device_id={"seq": peer}, device_id_type=MESH)
    for copy in small:
        copy.start()
    for j in range(runs):
        load_run(j).start()
    small[0].wait()
    pl.semaphore_wait(barrier, n - 1)

    def q_copy(slot, peer):
        return pltpu.make_async_remote_copy(
            src_ref=q_all.at[slot], dst_ref=q_all.at[slot], send_sem=q_send.at[peer],
            recv_sem=q_recv.at[slot], device_id={"seq": peer}, device_id_type=MESH,
        )

    for peer in peers:
        q_copy(me, peer).start()
    for copy in small[1:]:
        copy.wait()

    table = pt_v[...]
    row_id = lax.broadcasted_iota(jnp.int32, (requests, ctx), 0)
    col_f = lax.broadcasted_iota(jnp.int32, (requests, ctx), 1).astype(F32)
    len_grid = jnp.zeros((requests, ctx), F32)
    for r in range(requests):
        len_grid = jnp.where(row_id == r, len_s[r].astype(F32), len_grid)
    head_row = lax.broadcasted_iota(jnp.int32, (heads, 1), 0)
    head_id = lax.rem(head_row, n) * per_dev + head_row // n
    kv_row = head_id // group
    chosen_ids = []
    for r in range(requests):
        ids = sel_v[r].astype(F32)
        wide = jnp.zeros((heads, ids.shape[1]), F32)
        for k in range(kv_heads):
            wide = jnp.where(kv_row == k, ids[k : k + 1, :], wide)
        chosen_ids.append(wide)
    lane = lax.broadcasted_iota(jnp.int32, (1, span), 1)
    lane_f = lane.astype(F32)
    hot, valid, fine_ok, live, count = [], [], [], [], []
    for j in range(runs):
        match = table == me * slots + j * RUN
        page = jnp.sum(jnp.where(match, col_f, 0.0), axis=(0, 1), keepdims=True)
        length = jnp.sum(jnp.where(match, len_grid, 0.0), axis=(0, 1), keepdims=True)
        owner = jnp.max(jnp.where(match, 1.0, 0.0), axis=1, keepdims=True)
        hot_j = [owner[r : r + 1, :] for r in range(requests)]
        ids = chosen_ids[0] * hot_j[0]
        for r in range(1, requests):
            ids = ids + chosen_ids[r] * hot_j[r]
        valid_j = jnp.where(page * page_len + lane_f < length, 1.0, 0.0)
        ok = jnp.zeros((heads, span), F32)
        live_j, count_j = [], []
        for e in range(RUN):
            hit = jnp.max(jnp.where(ids == page + e, 1.0, 0.0), axis=1, keepdims=True)
            ok = jnp.where(lane // page_len == e, hit, ok)
            left = length - (page + e) * page_len
            live_j.append(jnp.where(left > 0.0, 1.0, 0.0))
            count_j.append(jnp.clip(left, 1.0, float(page_len)))
        hot.append(hot_j)
        valid.append(valid_j)
        fine_ok.append(ok * valid_j)
        live.append(live_j)
        count.append(count_j)

    row16 = lax.broadcasted_iota(jnp.int32, (16, span), 0)

    def by_head(row):
        wide = jnp.broadcast_to(row[:, :HEAD_DIM], (heads, HEAD_DIM))
        for k in range(1, kv_heads):
            wide = jnp.where(kv_row == k, row[:, k * HEAD_DIM : (k + 1) * HEAD_DIM], wide)
        return wide

    for j in range(runs):
        load_run(j).wait()
        page_rows = jnp.where(lane // page_len == row16, valid[j], 0.0).astype(BF16)
        sums = jnp.dot(
            page_rows, kv_buf[j * RUN : (j + 1) * RUN].reshape(span, width),
            preferred_element_type=F32,
        )
        for e in range(RUN):
            mean = (sums[e : e + 1, :] / count[j][e]).astype(BF16).astype(F32)
            sum_k[j * RUN + e] = by_head(mean[:, :kv_width])
            sum_v[j * RUN + e] = by_head(mean[:, kv_width:])

    for step, peer in enumerate(peers):
        q_copy(peer, peer).wait_recv()
    for src in range(n):
        rows = q_all[src].astype(F32)
        for w in range(per_dev):
            q_even[w, src * requests : (src + 1) * requests, :] = rows[
                :, w * HEAD_DIM : (w + 1) * HEAD_DIM
            ]
    q_rows = [
        jnp.concatenate(
            [q_even[w, pl.ds(r, n, stride=requests), :] for w in range(per_dev)], axis=0
        )
        for r in range(requests)
    ]
    kv_col = jnp.broadcast_to(kv_row, (heads, HEAD_DIM))
    own = [jnp.where(kv_col == k, 1.0, 0.0).astype(BF16) for k in range(kv_heads)]

    scores, coarse_s = [], []
    for j in range(runs):
        q_j = q_rows[0] * hot[j][0]
        for r in range(1, requests):
            q_j = q_j + q_rows[r] * hot[j][r]
        q_b = q_j.astype(BF16)
        q_bd = jnp.concatenate([q_b * own[k] for k in range(kv_heads)], axis=1)
        keys = kv_buf[j * RUN : (j + 1) * RUN, :, :kv_width].reshape(span, kv_width)
        scores.append(
            lax.dot_general(
                q_bd, keys, (((1,), (1,)), ((), ())), preferred_element_type=F32
            )
        )
        pair = []
        for e in range(RUN):
            dot = jnp.sum(q_j * sum_k[j * RUN + e], axis=1, keepdims=True) * scale
            pair.append(jnp.where(live[j][e] > 0.0, dot, neg_big))
        coarse_s.append(pair)
    kind_rows = per_dev * requests
    rows_out = kind_rows + 1
    lane_id = lax.broadcasted_iota(jnp.int32, (n, HEAD_DIM), 1)

    def request_tops(run_tops):
        tops = []
        for r in range(requests):
            held = [jnp.where(hot[j][r] > 0.0, run_tops[j], neg_big) for j in range(runs)]
            tops.append(functools.reduce(jnp.maximum, held).astype(BF16).astype(F32))
        return tops

    def of_run(tops, j):
        mine = tops[0] * hot[j][0]
        for r in range(1, requests):
            mine = mine + tops[r] * hot[j][r]
        return mine

    def weight_of(score, base):
        return jnp.where(score > 0.5 * neg_big, jnp.exp2(score - base), 0.0)

    def split_by_request(parts):
        totals = []
        for r in range(requests):
            total = parts[0] * hot[0][r]
            for j in range(1, runs):
                total = total + parts[j] * hot[j][r]
            totals.append(total)
        return totals

    coarse_tops = request_tops([functools.reduce(jnp.maximum, pair) for pair in coarse_s])
    coarse_sum, coarse_num = [], []
    for j in range(runs):
        base = of_run(coarse_tops, j)
        wts = [weight_of(s, base) for s in coarse_s[j]]
        coarse_sum.append(functools.reduce(jnp.add, wts))
        coarse_num.append(
            functools.reduce(jnp.add, [wts[e] * sum_v[j * RUN + e] for e in range(RUN)])
        )
    def p_copy(kind, slot, peer):
        return pltpu.make_async_remote_copy(
            src_ref=send_buf.at[kind, peer], dst_ref=recv_buf.at[kind, slot],
            send_sem=p_send.at[kind, peer], recv_sem=p_recv.at[kind, slot],
            device_id={"seq": peer}, device_id_type=MESH,
        )

    def send_partials(kind, tops, sums, nums):
        stat = jnp.zeros((n, HEAD_DIM), F32)
        for r in range(requests):
            high = sums[r].astype(BF16).astype(F32)
            for w in range(per_dev):
                part = slice(w * n, (w + 1) * n)
                row = w * requests + r
                gather_f[pl.ds(row, n, stride=rows_out), :] = nums[r][part]
                for i, value in enumerate((tops[r], high, sums[r] - high)):
                    stat = jnp.where(lane_id == i * kind_rows + row, value[part], stat)
        gather_f[pl.ds(kind_rows, n, stride=rows_out), :] = stat
        for d in range(n):
            send_buf[kind, d] = gather_f[d * rows_out : (d + 1) * rows_out, :].astype(BF16)
        for peer in peers:
            p_copy(kind, me, peer).start()
        recv_buf[kind, me] = send_buf[kind, me]

    send_partials(0, coarse_tops, split_by_request(coarse_sum), split_by_request(coarse_num))

    fine_m, fine_l, weights = [], [], []
    for j in range(runs):
        ok = fine_ok[j] > 0.0
        masked = jnp.where(ok, scores[j] * scale, neg_big)
        top = jnp.max(masked, axis=1, keepdims=True)
        wt = jnp.where(ok, jnp.exp2(masked - top), 0.0).astype(BF16)
        fine_m.append(top)
        fine_l.append(jnp.sum(wt.astype(F32), axis=1, keepdims=True))
        weights.append(wt)
    fine_n = []
    for j in range(runs):
        vals = kv_buf[j * RUN : (j + 1) * RUN, :, kv_width:].reshape(span, kv_width)
        mixed = jnp.dot(weights[j], vals, preferred_element_type=F32)
        num = mixed[:, :HEAD_DIM]
        for k in range(1, kv_heads):
            num = jnp.where(kv_row == k, mixed[:, k * HEAD_DIM : (k + 1) * HEAD_DIM], num)
        fine_n.append(num)

    fine_tops = request_tops(fine_m)
    fine_sum, fine_num = [], []
    for j in range(runs):
        wt = weight_of(fine_m[j], of_run(fine_tops, j))
        fine_sum.append(wt * fine_l[j])
        fine_num.append(wt * fine_n[j])
    send_partials(1, fine_tops, split_by_request(fine_sum), split_by_request(fine_num))

    gates = jax.nn.sigmoid(gate_v[...])
    gate_lane = lax.broadcasted_iota(jnp.int32, gates.shape, 1)
    gate_col = [
        [
            jnp.sum(
                jnp.where(gate_lane == kind * heads + me * per_dev + w, gates, 0.0),
                axis=1, keepdims=True,
            )
            for w in range(per_dev)
        ]
        for kind in range(2)
    ]
    full = []
    for kind in range(2):
        for peer in peers:
            p_copy(kind, peer, peer).wait_recv()
        stats = jnp.concatenate(
            [recv_buf[kind, src, kind_rows:, :].astype(F32) for src in range(n)], axis=0
        )
        tops = stats[:, :kind_rows]
        weight = jnp.exp2(tops - jnp.max(tops, axis=0, keepdims=True))
        both = stats[:, kind_rows : 2 * kind_rows] + stats[:, 2 * kind_rows : 3 * kind_rows]
        weight = weight / jnp.sum(weight * both, axis=0, keepdims=True)
        weight = weight.T
        num = jnp.zeros((kind_rows, HEAD_DIM), F32)
        for src in range(n):
            num = num + weight[:, src : src + 1] * recv_buf[kind, src, :kind_rows, :].astype(F32)
        full.append(num)
    for w in range(per_dev):
        part = slice(w * requests, (w + 1) * requests)
        out_ref[:, w * HEAD_DIM : (w + 1) * HEAD_DIM] = (
            gate_col[0][w] * full[0][part] + gate_col[1][w] * full[1][part]
        ).astype(BF16)
    for peer in peers:
        q_copy(me, peer).wait_send()
        p_copy(0, me, peer).wait_send()
        p_copy(1, me, peer).wait_send()


def per_device(queries, gate_logits, kv_pool, page_table, selected, lengths):
    n = lax.axis_size("seq")
    slots, page_len, width = kv_pool.shape
    requests, cols = queries.shape
    if cols % HEAD_DIM != 0:
        return per_device_plain(queries, gate_logits, kv_pool, page_table, selected, lengths)
    per_dev = cols // HEAD_DIM
    rows_out = per_dev * requests + 1
    dma = pltpu.SemaphoreType.DMA
    return pl.pallas_call(
        functools.partial(fused_kernel, n),
        out_shape=jax.ShapeDtypeStruct((requests, cols), BF16),
        in_specs=[pl.BlockSpec(memory_space=pltpu.HBM)] * 6,
        out_specs=pl.BlockSpec(memory_space=pltpu.VMEM),
        scratch_shapes=[
            pltpu.VMEM(kv_pool.shape, BF16),
            pltpu.VMEM((n, requests, cols), BF16),
            pltpu.VMEM(gate_logits.shape, F32),
            pltpu.VMEM(page_table.shape, jnp.int32),
            pltpu.VMEM(selected.shape, jnp.int32),
            pltpu.SMEM(lengths.shape, jnp.int32),
            pltpu.VMEM((per_dev, n * requests, HEAD_DIM), F32),
            pltpu.VMEM((slots, per_dev * n, HEAD_DIM), F32),
            pltpu.VMEM((slots, per_dev * n, HEAD_DIM), F32),
            pltpu.VMEM((n * rows_out, HEAD_DIM), F32),
            pltpu.VMEM((2, n, rows_out, HEAD_DIM), BF16),
            pltpu.VMEM((2, n, rows_out, HEAD_DIM), BF16),
            dma((slots // RUN,)),
            dma((5,)),
            dma((n,)),
            dma((n,)),
            dma((2, n)),
            dma((2, n)),
        ],
        compiler_params=pltpu.CompilerParams(
            collective_id=0, has_side_effects=True, vmem_limit_bytes=67043328
        ),
        name="paged_sparse_decode",
    )(queries, gate_logits, kv_pool, page_table, selected, lengths)


def solution(mesh):
    return jax.shard_map(
        per_device,
        mesh=mesh,
        in_specs=(
            P("grp", "seq"),
            P("grp", None),
            P(("grp", "seq"), None, None),
            P("grp", None),
            P("grp", None, None),
            P("grp"),
        ),
        out_specs=P("grp", "seq"),
        check_vma=False,
    )
```

```python
import functools
import math

import jax
import jax.numpy as jnp
from jax import lax
from jax.experimental import pallas as pl
from jax.experimental.pallas import tpu as pltpu
from jax.sharding import PartitionSpec as P

HEAD_DIM = 128


neg_big = -1e30


def joined(part, axis, combine):
    gathered = jax.tree.map(lambda a: lax.all_gather(a, axis), part)

    def take(source):
        return jax.tree.map(lambda a: lax.dynamic_index_in_dim(a, source, 0, False), gathered)

    return lax.fori_loop(
        1, lax.axis_size(axis), lambda source, state: combine(state, take(source)), take(0)
    )


def merge_pair(left, right):
    merged = ()
    for offset in (0, 3):
        row_top = jnp.maximum(left[offset], right[offset])
        left_scale = jnp.exp(left[offset] - row_top)
        right_scale = jnp.exp(right[offset] - row_top)
        merged = merged + (
            row_top,
            left[offset + 1] * left_scale + right[offset + 1] * right_scale,
            left[offset + 2] * left_scale[..., None] + right[offset + 2] * right_scale[..., None],
        )
    return merged


def per_device_plain(queries, gate_logits, kv_pool, page_table, selected, lengths):
    slot_count, page_len, double_width = kv_pool.shape
    kv_width = double_width // 2
    kv_heads = kv_width // HEAD_DIM
    requests = page_table.shape[0]
    ctx_pages = page_table.shape[1]
    col_count = queries.shape[1]
    highest = lax.Precision.HIGHEST
    all_queries = lax.all_gather(queries, "seq", axis=1, tiled=True)
    head_count = all_queries.shape[1] // HEAD_DIM
    group_size = head_count // kv_heads
    score_scale = 1.0 / math.sqrt(HEAD_DIM)
    first_slot = lax.axis_index("seq") * slot_count
    slot_ids = first_slot + jnp.arange(slot_count, dtype=jnp.int32)
    slot_match = page_table[:, :, None] == slot_ids[None, None, :]
    owner_hot = jnp.any(slot_match, axis=1)
    page_index = jnp.arange(ctx_pages, dtype=jnp.int32)
    page_of = jnp.sum(jnp.where(slot_match, page_index[None, :, None], 0), axis=(0, 1))
    slot_len = jnp.sum(jnp.where(owner_hot, lengths[:, None], 0), axis=0)
    owner_rows = jnp.dot(
        owner_hot.T.astype(jnp.bfloat16), all_queries, preferred_element_type=jnp.float32
    ).astype(jnp.bfloat16)
    slot_queries = owner_rows.reshape(slot_count, kv_heads, group_size, HEAD_DIM)
    key_rows = kv_pool[:, :, :kv_width].reshape(slot_count, page_len, kv_heads, HEAD_DIM)
    value_rows = kv_pool[:, :, kv_width:].reshape(slot_count, page_len, kv_heads, HEAD_DIM)
    position = page_of[:, None] * page_len + jnp.arange(page_len, dtype=jnp.int32)[None, :]
    is_valid = position < slot_len[:, None]
    is_live = page_of * page_len < slot_len
    valid_bf = is_valid.astype(jnp.bfloat16)
    counts = jnp.maximum(jnp.sum(is_valid.astype(jnp.float32), axis=1), 1.0)
    summary_keys = (
        jnp.einsum("st,stkd->skd", valid_bf, key_rows, preferred_element_type=jnp.float32)
        / counts[:, None, None]
    ).astype(jnp.bfloat16)
    summary_values = (
        jnp.einsum("st,stkd->skd", valid_bf, value_rows, preferred_element_type=jnp.float32)
        / counts[:, None, None]
    ).astype(jnp.bfloat16)
    coarse = (
        jnp.einsum("skgd,skd->skg", slot_queries, summary_keys, preferred_element_type=jnp.float32)
        * score_scale
    )
    coarse_mask = owner_hot[:, :, None, None] & is_live[None, :, None, None]
    coarse_masked = jnp.where(coarse_mask, coarse[None], neg_big)
    coarse_top = jnp.max(coarse_masked, axis=1)
    coarse_wt = jnp.where(coarse_mask, jnp.exp(coarse_masked - coarse_top[:, None]), 0.0)
    coarse_sum = jnp.sum(coarse_wt, axis=1)
    coarse_num = jnp.einsum(
        "rskg,skd->rkgd", coarse_wt, summary_values.astype(jnp.float32), precision=highest
    )
    fine_scores = (
        jnp.einsum("skgd,stkd->skgt", slot_queries, key_rows, preferred_element_type=jnp.float32)
        * score_scale
    )
    token_mask = is_valid[:, None, None, :]
    fine_masked = jnp.where(token_mask, fine_scores, neg_big)
    page_max = jnp.max(fine_masked, axis=3)
    page_wt = jnp.where(token_mask, jnp.exp(fine_masked - page_max[..., None]), 0.0).astype(
        jnp.bfloat16
    )
    page_sum = jnp.sum(page_wt.astype(jnp.float32), axis=3)
    page_num = jnp.einsum(
        "skgt,stkd->skgd", page_wt, value_rows, preferred_element_type=jnp.float32
    )
    page_hit = selected[:, None, :, :] == page_of[None, :, None, None]
    chosen = jnp.any(page_hit, axis=3) & owner_hot[:, :, None]
    chosen_full = chosen[..., None]
    sel_masked = jnp.where(chosen_full, page_max[None], neg_big)
    fine_top = jnp.max(sel_masked, axis=1)
    fine_wt = jnp.where(chosen_full, jnp.exp(sel_masked - fine_top[:, None]), 0.0)
    fine_sum = jnp.sum(fine_wt * page_sum[None], axis=1)
    fine_num = jnp.einsum("rskg,skgd->rkgd", fine_wt, page_num, precision=highest)
    gate_all = jax.nn.sigmoid(gate_logits)
    start_col = lax.axis_index("seq") * col_count
    coarse_gate = lax.dynamic_slice_in_dim(
        jnp.repeat(gate_all[:, :head_count], HEAD_DIM, axis=1), start_col, col_count, 1
    )
    fine_gate = lax.dynamic_slice_in_dim(
        jnp.repeat(gate_all[:, head_count:], HEAD_DIM, axis=1), start_col, col_count, 1
    )
    merged = joined(
        (coarse_top, coarse_sum, coarse_num, fine_top, fine_sum, fine_num), "seq", merge_pair
    )
    coarse_full = (merged[2] / merged[1][..., None]).reshape(requests, head_count * HEAD_DIM)
    fine_full = (merged[5] / merged[4][..., None]).reshape(requests, head_count * HEAD_DIM)
    coarse_cols = lax.dynamic_slice_in_dim(coarse_full, start_col, col_count, 1)
    fine_cols = lax.dynamic_slice_in_dim(fine_full, start_col, col_count, 1)
    return (coarse_gate * coarse_cols + fine_gate * fine_cols).astype(jnp.bfloat16)


RUN = 2
MESH = pl.DeviceIdType.MESH
F32 = jnp.float32
BF16 = jnp.bfloat16


def fused_kernel(
    n, q_hbm, gate_hbm, kv_hbm, pt_hbm, sel_hbm, len_hbm, out_ref,
    kv_buf, q_all, gate_v, pt_v, sel_v, len_s, q_even, score_v, sum_k, sum_v, gather_f, send_buf, recv_buf,
    kv_sem, in_sem, q_send, q_recv, p_send, p_recv,
):
    me = lax.axis_index("seq")
    slots, page_len, width = kv_buf.shape
    kv_width = width // 2
    kv_heads = kv_width // HEAD_DIM
    runs = slots // RUN
    span = RUN * page_len
    requests, ctx = pt_v.shape
    per_dev = q_all.shape[2] // HEAD_DIM
    heads = per_dev * n
    group = heads // kv_heads
    scale = math.log2(math.e) / math.sqrt(HEAD_DIM)

    def load_run(j):
        return pltpu.make_async_copy(
            kv_hbm.at[pl.ds(j * RUN, RUN)], kv_buf.at[pl.ds(j * RUN, RUN)], kv_sem.at[j]
        )

    small = [
        pltpu.make_async_copy(q_hbm, q_all.at[me], in_sem.at[0]),
        pltpu.make_async_copy(pt_hbm, pt_v, in_sem.at[1]),
        pltpu.make_async_copy(len_hbm, len_s, in_sem.at[2]),
        pltpu.make_async_copy(sel_hbm, sel_v, in_sem.at[3]),
        pltpu.make_async_copy(gate_hbm, gate_v, in_sem.at[4]),
    ]
    barrier = pltpu.get_barrier_semaphore()
    peers = [
        lax.rem(me + step, n) for step in sorted(range(1, n), key=lambda s: min(s, n - s))
    ]
    for peer in peers:
        pl.semaphore_signal(barrier, inc=1, device_id={"seq": peer}, device_id_type=MESH)
    for copy in small:
        copy.start()
    for j in range(runs):
        load_run(j).start()
    small[0].wait()
    pl.semaphore_wait(barrier, n - 1)

    def q_copy(slot, peer):
        return pltpu.make_async_remote_copy(
            src_ref=q_all.at[slot], dst_ref=q_all.at[slot], send_sem=q_send.at[peer],
            recv_sem=q_recv.at[slot], device_id={"seq": peer}, device_id_type=MESH,
        )

    for peer in peers:
        q_copy(me, peer).start()
    for copy in small[1:]:
        copy.wait()

    table = pt_v[...]
    row_id = lax.broadcasted_iota(jnp.int32, (requests, ctx), 0)
    col_f = lax.broadcasted_iota(jnp.int32, (requests, ctx), 1).astype(F32)
    len_grid = jnp.zeros((requests, ctx), F32)
    for r in range(requests):
        len_grid = jnp.where(row_id == r, len_s[r].astype(F32), len_grid)
    head_row = lax.broadcasted_iota(jnp.int32, (heads, 1), 0)
    head_id = lax.rem(head_row, n) * per_dev + head_row // n
    kv_row = head_id // group
    chosen_ids = []
    for r in range(requests):
        ids = sel_v[r].astype(F32)
        wide = jnp.zeros((heads, ids.shape[1]), F32)
        for k in range(kv_heads):
            wide = jnp.where(kv_row == k, ids[k : k + 1, :], wide)
        chosen_ids.append(wide)
    lane = lax.broadcasted_iota(jnp.int32, (1, span), 1)
    lane_f = lane.astype(F32)
    hot, valid, fine_ok, live, count = [], [], [], [], []
    for j in range(runs):
        match = table == me * slots + j * RUN
        page = jnp.sum(jnp.where(match, col_f, 0.0), axis=(0, 1), keepdims=True)
        length = jnp.sum(jnp.where(match, len_grid, 0.0), axis=(0, 1), keepdims=True)
        owner = jnp.max(jnp.where(match, 1.0, 0.0), axis=1, keepdims=True)
        hot_j = [owner[r : r + 1, :] for r in range(requests)]
        ids = chosen_ids[0] * hot_j[0]
        for r in range(1, requests):
            ids = ids + chosen_ids[r] * hot_j[r]
        valid_j = jnp.where(page * page_len + lane_f < length, 1.0, 0.0)
        ok = jnp.zeros((heads, span), F32)
        live_j, count_j = [], []
        for e in range(RUN):
            hit = jnp.max(jnp.where(ids == page + e, 1.0, 0.0), axis=1, keepdims=True)
            ok = jnp.where(lane // page_len == e, hit, ok)
            left = length - (page + e) * page_len
            live_j.append(jnp.where(left > 0.0, 1.0, 0.0))
            count_j.append(jnp.clip(left, 1.0, float(page_len)))
        hot.append(hot_j)
        valid.append(valid_j)
        fine_ok.append(ok * valid_j)
        live.append(live_j)
        count.append(count_j)

    row16 = lax.broadcasted_iota(jnp.int32, (16, span), 0)

    def by_head(row):
        wide = jnp.broadcast_to(row[:, :HEAD_DIM], (heads, HEAD_DIM))
        for k in range(1, kv_heads):
            wide = jnp.where(kv_row == k, row[:, k * HEAD_DIM : (k + 1) * HEAD_DIM], wide)
        return wide

    for j in range(runs):
        load_run(j).wait()
        page_rows = jnp.where(lane // page_len == row16, valid[j], 0.0).astype(BF16)
        sums = jnp.dot(
            page_rows, kv_buf[j * RUN : (j + 1) * RUN].reshape(span, width),
            preferred_element_type=F32,
        )
        for e in range(RUN):
            mean = (sums[e : e + 1, :] / count[j][e]).astype(BF16).astype(F32)
            sum_k[j * RUN + e] = by_head(mean[:, :kv_width])
            sum_v[j * RUN + e] = by_head(mean[:, kv_width:])

    half = n // 2
    half_heads = kv_heads // 2
    half_width = half_heads * HEAD_DIM
    my_half = me // half
    half_row = lax.broadcasted_iota(jnp.int32, (per_dev * half, HEAD_DIM), 0)
    half_kv = (lax.rem(half_row, half) * per_dev + half_row // half) // group
    own = [jnp.where(half_kv == k, 1.0, 0.0).astype(BF16) for k in range(half_heads)]
    parts = []
    for stage in range(2):
        which = my_half if stage == 0 else 1 - my_half
        if stage == 0:
            for step in range(1, half):
                near = my_half * half + lax.rem(lax.rem(me, half) + step, half)
                q_copy(near, near).wait_recv()
        else:
            for i in range(half):
                q_copy(which * half + i, which * half + i).wait_recv()
        for i in range(half):
            rows = q_all[which * half + i].astype(F32)
            for w in range(per_dev):
                q_even[stage, w, i * requests : (i + 1) * requests, :] = rows[
                    :, w * HEAD_DIM : (w + 1) * HEAD_DIM
                ]
        part = [
            jnp.concatenate(
                [q_even[stage, w, pl.ds(r, half, stride=requests), :] for w in range(per_dev)],
                axis=0,
            )
            for r in range(requests)
        ]
        parts.append(part)
        first_col = pl.multiple_of(which * half_width, half_width)
        for j in range(runs):
            q_j = part[0] * hot[j][0]
            for r in range(1, requests):
                q_j = q_j + part[r] * hot[j][r]
            q_b = q_j.astype(BF16)
            q_bd = jnp.concatenate([q_b * own[k] for k in range(half_heads)], axis=1)
            keys = kv_buf[j * RUN : (j + 1) * RUN, :, pl.ds(first_col, half_width)]
            dots = lax.dot_general(
                q_bd, keys.reshape(span, half_width), (((1,), (1,)), ((), ())),
                preferred_element_type=F32,
            )
            for w in range(per_dev):
                score_v[j, pl.ds(pl.multiple_of(w * n + which * half, 8), half), :] = dots[
                    w * half : (w + 1) * half
                ]
    q_rows = []
    for r in range(requests):
        pieces = []
        for w in range(per_dev):
            near, far = [parts[stage][r][w * half : (w + 1) * half] for stage in range(2)]
            pieces.append(jnp.where(my_half == 0, near, far))
            pieces.append(jnp.where(my_half == 0, far, near))
        q_rows.append(jnp.concatenate(pieces, axis=0))

    scores, coarse_s = [], []
    for j in range(runs):
        q_j = q_rows[0] * hot[j][0]
        for r in range(1, requests):
            q_j = q_j + q_rows[r] * hot[j][r]
        scores.append(score_v[j])
        pair = []
        for e in range(RUN):
            dot = jnp.sum(q_j * sum_k[j * RUN + e], axis=1, keepdims=True) * scale
            pair.append(jnp.where(live[j][e] > 0.0, dot, neg_big))
        coarse_s.append(pair)
    fine_m, fine_l, weights = [], [], []
    for j in range(runs):
        ok = fine_ok[j] > 0.0
        masked = jnp.where(ok, scores[j] * scale, neg_big)
        top = jnp.max(masked, axis=1, keepdims=True)
        wt = jnp.where(ok, jnp.exp2(masked - top), 0.0).astype(BF16)
        fine_m.append(top)
        fine_l.append(jnp.sum(wt.astype(F32), axis=1, keepdims=True))
        weights.append(wt)
    fine_n = []
    for j in range(runs):
        vals = kv_buf[j * RUN : (j + 1) * RUN, :, kv_width:].reshape(span, kv_width)
        mixed = jnp.dot(weights[j], vals, preferred_element_type=F32)
        num = mixed[:, :HEAD_DIM]
        for k in range(1, kv_heads):
            num = jnp.where(kv_row == k, mixed[:, k * HEAD_DIM : (k + 1) * HEAD_DIM], num)
        fine_n.append(num)

    kind_rows = per_dev * requests
    unit = 2 * kind_rows
    rows_out = unit + kind_rows
    lane_id = lax.broadcasted_iota(jnp.int32, (heads, HEAD_DIM), 1)

    def request_tops(run_tops):
        tops = []
        for r in range(requests):
            held = [jnp.where(hot[j][r] > 0.0, run_tops[j], neg_big) for j in range(runs)]
            tops.append(functools.reduce(jnp.maximum, held).astype(BF16).astype(F32))
        return tops

    def of_run(tops, j):
        mine = tops[0] * hot[j][0]
        for r in range(1, requests):
            mine = mine + tops[r] * hot[j][r]
        return mine

    def weight_of(score, base):
        return jnp.where(score > 0.5 * neg_big, jnp.exp2(score - base), 0.0)

    def split_by_request(parts):
        totals = []
        for r in range(requests):
            total = parts[0] * hot[0][r]
            for j in range(1, runs):
                total = total + parts[j] * hot[j][r]
            totals.append(total)
        return totals

    coarse_tops = request_tops([functools.reduce(jnp.maximum, pair) for pair in coarse_s])
    coarse_sum, coarse_num = [], []
    for j in range(runs):
        base = of_run(coarse_tops, j)
        wts = [weight_of(s, base) for s in coarse_s[j]]
        coarse_sum.append(functools.reduce(jnp.add, wts))
        coarse_num.append(
            functools.reduce(jnp.add, [wts[e] * sum_v[j * RUN + e] for e in range(RUN)])
        )
    fine_tops = request_tops(fine_m)
    fine_sum, fine_num = [], []
    for j in range(runs):
        wt = weight_of(fine_m[j], of_run(fine_tops, j))
        fine_sum.append(wt * fine_l[j])
        fine_num.append(wt * fine_n[j])
    tops = [coarse_tops, fine_tops]
    sums = [split_by_request(coarse_sum), split_by_request(fine_sum)]
    nums = [split_by_request(coarse_num), split_by_request(fine_num)]
    for r in range(requests):
        stat = jnp.zeros((heads, HEAD_DIM), F32)
        for kind in range(2):
            high = sums[kind][r].astype(BF16).astype(F32)
            for i, value in enumerate((tops[kind][r], high, sums[kind][r] - high)):
                stat = jnp.where(lane_id == 3 * kind + i, value, stat)
        for w in range(per_dev):
            part = slice(w * n, (w + 1) * n)
            row = w * requests + r
            for kind in range(2):
                gather_f[pl.ds(kind * kind_rows + row, n, stride=rows_out), :] = nums[kind][r][part]
            gather_f[pl.ds(unit + row, n, stride=rows_out), :] = stat[part]
    for d in range(n):
        send_buf[d] = gather_f[d * rows_out : (d + 1) * rows_out, :].astype(BF16)

    def p_copy(slot, peer):
        return pltpu.make_async_remote_copy(
            src_ref=send_buf.at[peer], dst_ref=recv_buf.at[slot], send_sem=p_send.at[peer],
            recv_sem=p_recv.at[slot], device_id={"seq": peer}, device_id_type=MESH,
        )

    for peer in peers:
        p_copy(me, peer).start()
    recv_buf[me] = send_buf[me]
    gates = jax.nn.sigmoid(gate_v[...])
    gate_lane = lax.broadcasted_iota(jnp.int32, gates.shape, 1)
    gate_col = [
        [
            jnp.sum(
                jnp.where(gate_lane == kind * heads + me * per_dev + w, gates, 0.0),
                axis=1, keepdims=True,
            )
            for w in range(per_dev)
        ]
        for kind in range(2)
    ]
    for peer in peers:
        p_copy(peer, peer).wait_recv()
    stats = [recv_buf[src, unit:, :].astype(F32) for src in range(n)]
    full = []
    for kind in range(2):
        tops = [s[:, 3 * kind : 3 * kind + 1] for s in stats]
        top = functools.reduce(jnp.maximum, tops)
        total = jnp.zeros((kind_rows, 1), F32)
        num = jnp.zeros((kind_rows, HEAD_DIM), F32)
        part = slice(kind * kind_rows, (kind + 1) * kind_rows)
        for src in range(n):
            weight = jnp.exp2(tops[src] - top)
            both = stats[src][:, 3 * kind + 1 : 3 * kind + 2] + stats[src][:, 3 * kind + 2 : 3 * kind + 3]
            total = total + weight * both
            num = num + weight * recv_buf[src, part, :].astype(F32)
        full.append(num / total)
    for w in range(per_dev):
        part = slice(w * requests, (w + 1) * requests)
        out_ref[:, w * HEAD_DIM : (w + 1) * HEAD_DIM] = (
            gate_col[0][w] * full[0][part] + gate_col[1][w] * full[1][part]
        ).astype(BF16)
    for peer in peers:
        q_copy(me, peer).wait_send()
        p_copy(me, peer).wait_send()


def per_device(queries, gate_logits, kv_pool, page_table, selected, lengths):
    n = lax.axis_size("seq")
    slots, page_len, width = kv_pool.shape
    requests, cols = queries.shape
    if cols % HEAD_DIM != 0 or n % 16 != 0:
        return per_device_plain(queries, gate_logits, kv_pool, page_table, selected, lengths)
    per_dev = cols // HEAD_DIM
    rows_out = 3 * per_dev * requests
    dma = pltpu.SemaphoreType.DMA
    return pl.pallas_call(
        functools.partial(fused_kernel, n),
        out_shape=jax.ShapeDtypeStruct((requests, cols), BF16),
        in_specs=[pl.BlockSpec(memory_space=pltpu.HBM)] * 6,
        out_specs=pl.BlockSpec(memory_space=pltpu.VMEM),
        scratch_shapes=[
            pltpu.VMEM(kv_pool.shape, BF16),
            pltpu.VMEM((n, requests, cols), BF16),
            pltpu.VMEM(gate_logits.shape, F32),
            pltpu.VMEM(page_table.shape, jnp.int32),
            pltpu.VMEM(selected.shape, jnp.int32),
            pltpu.SMEM(lengths.shape, jnp.int32),
            pltpu.VMEM((2, per_dev, n // 2 * requests, HEAD_DIM), F32),
            pltpu.VMEM((slots // RUN, per_dev * n, RUN * page_len), F32),
            pltpu.VMEM((slots, per_dev * n, HEAD_DIM), F32),
            pltpu.VMEM((slots, per_dev * n, HEAD_DIM), F32),
            pltpu.VMEM((n * rows_out, HEAD_DIM), F32),
            pltpu.VMEM((n, rows_out, HEAD_DIM), BF16),
            pltpu.VMEM((n, rows_out, HEAD_DIM), BF16),
            dma((slots // RUN,)),
            dma((5,)),
            dma((n,)),
            dma((n,)),
            dma((n,)),
            dma((n,)),
        ],
        compiler_params=pltpu.CompilerParams(
            collective_id=0, has_side_effects=True, vmem_limit_bytes=67043328
        ),
        name="paged_sparse_decode",
    )(queries, gate_logits, kv_pool, page_table, selected, lengths)


def solution(mesh):
    return jax.shard_map(
        per_device,
        mesh=mesh,
        in_specs=(
            P("grp", "seq"),
            P("grp", None),
            P(("grp", "seq"), None, None),
            P("grp", None),
            P("grp", None, None),
            P("grp"),
        ),
        out_specs=P("grp", "seq"),
        check_vma=False,
    )
```

```python
import functools
import math

import jax
import jax.numpy as jnp
from jax import lax
from jax.experimental import pallas as pl
from jax.experimental.pallas import tpu as pltpu
from jax.sharding import PartitionSpec as P

HEAD_DIM = 128


neg_big = -1e30


def joined(part, axis, combine):
    gathered = jax.tree.map(lambda a: lax.all_gather(a, axis), part)

    def take(source):
        return jax.tree.map(lambda a: lax.dynamic_index_in_dim(a, source, 0, False), gathered)

    return lax.fori_loop(
        1, lax.axis_size(axis), lambda source, state: combine(state, take(source)), take(0)
    )


def merge_pair(left, right):
    merged = ()
    for offset in (0, 3):
        row_top = jnp.maximum(left[offset], right[offset])
        left_scale = jnp.exp(left[offset] - row_top)
        right_scale = jnp.exp(right[offset] - row_top)
        merged = merged + (
            row_top,
            left[offset + 1] * left_scale + right[offset + 1] * right_scale,
            left[offset + 2] * left_scale[..., None] + right[offset + 2] * right_scale[..., None],
        )
    return merged


def per_device_plain(queries, gate_logits, kv_pool, page_table, selected, lengths):
    slot_count, page_len, double_width = kv_pool.shape
    kv_width = double_width // 2
    kv_heads = kv_width // HEAD_DIM
    requests = page_table.shape[0]
    ctx_pages = page_table.shape[1]
    col_count = queries.shape[1]
    highest = lax.Precision.HIGHEST
    all_queries = lax.all_gather(queries, "seq", axis=1, tiled=True)
    head_count = all_queries.shape[1] // HEAD_DIM
    group_size = head_count // kv_heads
    score_scale = 1.0 / math.sqrt(HEAD_DIM)
    first_slot = lax.axis_index("seq") * slot_count
    slot_ids = first_slot + jnp.arange(slot_count, dtype=jnp.int32)
    slot_match = page_table[:, :, None] == slot_ids[None, None, :]
    owner_hot = jnp.any(slot_match, axis=1)
    page_index = jnp.arange(ctx_pages, dtype=jnp.int32)
    page_of = jnp.sum(jnp.where(slot_match, page_index[None, :, None], 0), axis=(0, 1))
    slot_len = jnp.sum(jnp.where(owner_hot, lengths[:, None], 0), axis=0)
    owner_rows = jnp.dot(
        owner_hot.T.astype(jnp.bfloat16), all_queries, preferred_element_type=jnp.float32
    ).astype(jnp.bfloat16)
    slot_queries = owner_rows.reshape(slot_count, kv_heads, group_size, HEAD_DIM)
    key_rows = kv_pool[:, :, :kv_width].reshape(slot_count, page_len, kv_heads, HEAD_DIM)
    value_rows = kv_pool[:, :, kv_width:].reshape(slot_count, page_len, kv_heads, HEAD_DIM)
    position = page_of[:, None] * page_len + jnp.arange(page_len, dtype=jnp.int32)[None, :]
    is_valid = position < slot_len[:, None]
    is_live = page_of * page_len < slot_len
    valid_bf = is_valid.astype(jnp.bfloat16)
    counts = jnp.maximum(jnp.sum(is_valid.astype(jnp.float32), axis=1), 1.0)
    summary_keys = (
        jnp.einsum("st,stkd->skd", valid_bf, key_rows, preferred_element_type=jnp.float32)
        / counts[:, None, None]
    ).astype(jnp.bfloat16)
    summary_values = (
        jnp.einsum("st,stkd->skd", valid_bf, value_rows, preferred_element_type=jnp.float32)
        / counts[:, None, None]
    ).astype(jnp.bfloat16)
    coarse = (
        jnp.einsum("skgd,skd->skg", slot_queries, summary_keys, preferred_element_type=jnp.float32)
        * score_scale
    )
    coarse_mask = owner_hot[:, :, None, None] & is_live[None, :, None, None]
    coarse_masked = jnp.where(coarse_mask, coarse[None], neg_big)
    coarse_top = jnp.max(coarse_masked, axis=1)
    coarse_wt = jnp.where(coarse_mask, jnp.exp(coarse_masked - coarse_top[:, None]), 0.0)
    coarse_sum = jnp.sum(coarse_wt, axis=1)
    coarse_num = jnp.einsum(
        "rskg,skd->rkgd", coarse_wt, summary_values.astype(jnp.float32), precision=highest
    )
    fine_scores = (
        jnp.einsum("skgd,stkd->skgt", slot_queries, key_rows, preferred_element_type=jnp.float32)
        * score_scale
    )
    token_mask = is_valid[:, None, None, :]
    fine_masked = jnp.where(token_mask, fine_scores, neg_big)
    page_max = jnp.max(fine_masked, axis=3)
    page_wt = jnp.where(token_mask, jnp.exp(fine_masked - page_max[..., None]), 0.0).astype(
        jnp.bfloat16
    )
    page_sum = jnp.sum(page_wt.astype(jnp.float32), axis=3)
    page_num = jnp.einsum(
        "skgt,stkd->skgd", page_wt, value_rows, preferred_element_type=jnp.float32
    )
    page_hit = selected[:, None, :, :] == page_of[None, :, None, None]
    chosen = jnp.any(page_hit, axis=3) & owner_hot[:, :, None]
    chosen_full = chosen[..., None]
    sel_masked = jnp.where(chosen_full, page_max[None], neg_big)
    fine_top = jnp.max(sel_masked, axis=1)
    fine_wt = jnp.where(chosen_full, jnp.exp(sel_masked - fine_top[:, None]), 0.0)
    fine_sum = jnp.sum(fine_wt * page_sum[None], axis=1)
    fine_num = jnp.einsum("rskg,skgd->rkgd", fine_wt, page_num, precision=highest)
    gate_all = jax.nn.sigmoid(gate_logits)
    start_col = lax.axis_index("seq") * col_count
    coarse_gate = lax.dynamic_slice_in_dim(
        jnp.repeat(gate_all[:, :head_count], HEAD_DIM, axis=1), start_col, col_count, 1
    )
    fine_gate = lax.dynamic_slice_in_dim(
        jnp.repeat(gate_all[:, head_count:], HEAD_DIM, axis=1), start_col, col_count, 1
    )
    merged = joined(
        (coarse_top, coarse_sum, coarse_num, fine_top, fine_sum, fine_num), "seq", merge_pair
    )
    coarse_full = (merged[2] / merged[1][..., None]).reshape(requests, head_count * HEAD_DIM)
    fine_full = (merged[5] / merged[4][..., None]).reshape(requests, head_count * HEAD_DIM)
    coarse_cols = lax.dynamic_slice_in_dim(coarse_full, start_col, col_count, 1)
    fine_cols = lax.dynamic_slice_in_dim(fine_full, start_col, col_count, 1)
    return (coarse_gate * coarse_cols + fine_gate * fine_cols).astype(jnp.bfloat16)


RUN = 2
MESH = pl.DeviceIdType.MESH
F32 = jnp.float32
BF16 = jnp.bfloat16


def fused_kernel(
    n, q_hbm, gate_hbm, kv_hbm, pt_hbm, sel_hbm, len_hbm, out_ref,
    kv_buf, q_all, gate_v, pt_v, sel_v, len_s, q_even, mask_v, sum_k, sum_v, gather_f, send_buf, recv_buf,
    kv_sem, in_sem, q_send, q_recv, p_send, p_recv,
):
    me = lax.axis_index("seq")
    slots, page_len, width = kv_buf.shape
    kv_width = width // 2
    kv_heads = kv_width // HEAD_DIM
    runs = slots // RUN
    span = RUN * page_len
    requests, ctx = pt_v.shape
    per_dev = q_all.shape[2] // HEAD_DIM
    heads = per_dev * n
    group = heads // kv_heads
    scale = math.log2(math.e) / math.sqrt(HEAD_DIM)

    def load_run(j):
        return pltpu.make_async_copy(
            kv_hbm.at[pl.ds(j * RUN, RUN)], kv_buf.at[pl.ds(j * RUN, RUN)], kv_sem.at[j]
        )

    small = [
        pltpu.make_async_copy(q_hbm, q_all.at[me], in_sem.at[0]),
        pltpu.make_async_copy(pt_hbm, pt_v, in_sem.at[1]),
        pltpu.make_async_copy(len_hbm, len_s, in_sem.at[2]),
        pltpu.make_async_copy(sel_hbm, sel_v, in_sem.at[3]),
        pltpu.make_async_copy(gate_hbm, gate_v, in_sem.at[4]),
    ]
    barrier = pltpu.get_barrier_semaphore()
    peers = [
        lax.rem(me + step, n) for step in sorted(range(1, n), key=lambda s: min(s, n - s))
    ]
    for peer in peers:
        pl.semaphore_signal(barrier, inc=1, device_id={"seq": peer}, device_id_type=MESH)
    for copy in small:
        copy.start()
    for j in range(runs):
        load_run(j).start()
    small[0].wait()
    pl.semaphore_wait(barrier, n - 1)

    def q_copy(slot, peer):
        return pltpu.make_async_remote_copy(
            src_ref=q_all.at[slot], dst_ref=q_all.at[slot], send_sem=q_send.at[peer],
            recv_sem=q_recv.at[slot], device_id={"seq": peer}, device_id_type=MESH,
        )

    for peer in peers:
        q_copy(me, peer).start()
    for copy in small[1:]:
        copy.wait()

    table = pt_v[...]
    row_id = lax.broadcasted_iota(jnp.int32, (requests, ctx), 0)
    col_f = lax.broadcasted_iota(jnp.int32, (requests, ctx), 1).astype(F32)
    len_grid = jnp.zeros((requests, ctx), F32)
    for r in range(requests):
        len_grid = jnp.where(row_id == r, len_s[r].astype(F32), len_grid)
    head_row = lax.broadcasted_iota(jnp.int32, (heads, 1), 0)
    head_id = lax.rem(head_row, n) * per_dev + head_row // n
    kv_row = head_id // group
    chosen_ids = []
    for r in range(requests):
        ids = sel_v[r].astype(F32)
        wide = jnp.zeros((heads, ids.shape[1]), F32)
        for k in range(kv_heads):
            wide = jnp.where(kv_row == k, ids[k : k + 1, :], wide)
        chosen_ids.append(wide)
    lane = lax.broadcasted_iota(jnp.int32, (1, span), 1)
    lane_f = lane.astype(F32)
    hot, valid, live, count = [], [], [], []
    for j in range(runs):
        match = table == me * slots + j * RUN
        page = jnp.sum(jnp.where(match, col_f, 0.0), axis=(0, 1), keepdims=True)
        length = jnp.sum(jnp.where(match, len_grid, 0.0), axis=(0, 1), keepdims=True)
        owner = jnp.max(jnp.where(match, 1.0, 0.0), axis=1, keepdims=True)
        hot_j = [owner[r : r + 1, :] for r in range(requests)]
        ids = chosen_ids[0] * hot_j[0]
        for r in range(1, requests):
            ids = ids + chosen_ids[r] * hot_j[r]
        valid_j = jnp.where(page * page_len + lane_f < length, 1.0, 0.0)
        ok = jnp.zeros((heads, span), F32)
        live_j, count_j = [], []
        for e in range(RUN):
            hit = jnp.max(jnp.where(ids == page + e, 1.0, 0.0), axis=1, keepdims=True)
            ok = jnp.where(lane // page_len == e, hit, ok)
            left = length - (page + e) * page_len
            live_j.append(jnp.where(left > 0.0, 1.0, 0.0))
            count_j.append(jnp.clip(left, 1.0, float(page_len)))
        hot.append(hot_j)
        valid.append(valid_j)
        mask_v[j] = ok * valid_j
        live.append(live_j)
        count.append(count_j)

    row16 = lax.broadcasted_iota(jnp.int32, (16, span), 0)

    def by_head(row):
        wide = jnp.broadcast_to(row[:, :HEAD_DIM], (heads, HEAD_DIM))
        for k in range(1, kv_heads):
            wide = jnp.where(kv_row == k, row[:, k * HEAD_DIM : (k + 1) * HEAD_DIM], wide)
        return wide

    for j in range(runs):
        load_run(j).wait()
        page_rows = jnp.where(lane // page_len == row16, valid[j], 0.0).astype(BF16)
        sums = jnp.dot(
            page_rows, kv_buf[j * RUN : (j + 1) * RUN].reshape(span, width),
            preferred_element_type=F32,
        )
        for e in range(RUN):
            mean = (sums[e : e + 1, :] / count[j][e]).astype(BF16).astype(F32)
            sum_k[j * RUN + e] = by_head(mean[:, :kv_width])
            sum_v[j * RUN + e] = by_head(mean[:, kv_width:])

    half = n // 2
    half_heads = kv_heads // 2
    half_width = half_heads * HEAD_DIM
    my_half = me // half
    half_row = lax.broadcasted_iota(jnp.int32, (per_dev * half, HEAD_DIM), 0)
    half_kv = (lax.rem(half_row, half) * per_dev + half_row // half) // group
    own = [jnp.where(half_kv == k, 1.0, 0.0).astype(BF16) for k in range(half_heads)]
    parts, fine_parts = [], []
    for stage in range(2):
        which = my_half if stage == 0 else 1 - my_half
        if stage == 0:
            for step in range(1, half):
                near = my_half * half + lax.rem(lax.rem(me, half) + step, half)
                q_copy(near, near).wait_recv()
        else:
            for i in range(half):
                q_copy(which * half + i, which * half + i).wait_recv()
        for i in range(half):
            rows = q_all[which * half + i].astype(F32)
            for w in range(per_dev):
                q_even[stage, w, i * requests : (i + 1) * requests, :] = rows[
                    :, w * HEAD_DIM : (w + 1) * HEAD_DIM
                ]
        part = [
            jnp.concatenate(
                [q_even[stage, w, pl.ds(r, half, stride=requests), :] for w in range(per_dev)],
                axis=0,
            )
            for r in range(requests)
        ]
        parts.append(part)
        dots_all = []
        first_col = pl.multiple_of(which * half_width, half_width)
        for j in range(runs):
            q_j = part[0] * hot[j][0]
            for r in range(1, requests):
                q_j = q_j + part[r] * hot[j][r]
            q_b = q_j.astype(BF16)
            q_bd = jnp.concatenate([q_b * own[k] for k in range(half_heads)], axis=1)
            keys = kv_buf[j * RUN : (j + 1) * RUN, :, pl.ds(first_col, half_width)]
            dots = lax.dot_general(
                q_bd, keys.reshape(span, half_width), (((1,), (1,)), ((), ())),
                preferred_element_type=F32,
            )
            dots_all.append(dots)
        wts = []
        for j in range(runs):
            dots = dots_all[j]
            allowed = jnp.concatenate(
                [
                    mask_v[j, pl.ds(pl.multiple_of(w * n + which * half, 8), half), :]
                    for w in range(per_dev)
                ],
                axis=0,
            )
            ok = allowed > 0.0
            masked = jnp.where(ok, dots * scale, neg_big)
            top = jnp.max(masked, axis=1, keepdims=True)
            wt = jnp.where(ok, jnp.exp2(masked - top), 0.0).astype(BF16)
            total = jnp.sum(wt.astype(F32), axis=1, keepdims=True)
            wts.append((wt, top, total))
        for j in range(runs):
            wt, top, total = wts[j]
            vals = kv_buf[
                j * RUN : (j + 1) * RUN, :,
                pl.ds(pl.multiple_of(kv_width + which * half_width, half_width), half_width),
            ]
            mixed = jnp.dot(wt, vals.reshape(span, half_width), preferred_element_type=F32)
            num = mixed[:, :HEAD_DIM]
            for k in range(1, half_heads):
                num = jnp.where(half_kv == k, mixed[:, k * HEAD_DIM : (k + 1) * HEAD_DIM], num)
            fine_parts.append((top, total, num))

    def joined_halves(near, far):
        pieces = []
        for w in range(per_dev):
            part = slice(w * half, (w + 1) * half)
            pieces.append(jnp.where(my_half == 0, near[part], far[part]))
            pieces.append(jnp.where(my_half == 0, far[part], near[part]))
        return jnp.concatenate(pieces, axis=0)

    fine_m, fine_l, fine_n = [
        [joined_halves(fine_parts[j][i], fine_parts[runs + j][i]) for j in range(runs)]
        for i in range(3)
    ]
    q_rows = [joined_halves(parts[0][r], parts[1][r]) for r in range(requests)]

    coarse_s = []
    for j in range(runs):
        q_j = q_rows[0] * hot[j][0]
        for r in range(1, requests):
            q_j = q_j + q_rows[r] * hot[j][r]
        pair = []
        for e in range(RUN):
            dot = jnp.sum(q_j * sum_k[j * RUN + e], axis=1, keepdims=True) * scale
            pair.append(jnp.where(live[j][e] > 0.0, dot, neg_big))
        coarse_s.append(pair)
    kind_rows = per_dev * requests
    unit = 2 * kind_rows
    rows_out = unit + kind_rows
    lane_id = lax.broadcasted_iota(jnp.int32, (heads, HEAD_DIM), 1)

    def request_tops(run_tops):
        tops = []
        for r in range(requests):
            held = [jnp.where(hot[j][r] > 0.0, run_tops[j], neg_big) for j in range(runs)]
            tops.append(functools.reduce(jnp.maximum, held).astype(BF16).astype(F32))
        return tops

    def of_run(tops, j):
        mine = tops[0] * hot[j][0]
        for r in range(1, requests):
            mine = mine + tops[r] * hot[j][r]
        return mine

    def weight_of(score, base):
        return jnp.where(score > 0.5 * neg_big, jnp.exp2(score - base), 0.0)

    def split_by_request(parts):
        totals = []
        for r in range(requests):
            total = parts[0] * hot[0][r]
            for j in range(1, runs):
                total = total + parts[j] * hot[j][r]
            totals.append(total)
        return totals

    coarse_tops = request_tops([functools.reduce(jnp.maximum, pair) for pair in coarse_s])
    coarse_sum, coarse_num = [], []
    for j in range(runs):
        base = of_run(coarse_tops, j)
        wts = [weight_of(s, base) for s in coarse_s[j]]
        coarse_sum.append(functools.reduce(jnp.add, wts))
        coarse_num.append(
            functools.reduce(jnp.add, [wts[e] * sum_v[j * RUN + e] for e in range(RUN)])
        )
    fine_tops = request_tops(fine_m)
    fine_sum, fine_num = [], []
    for j in range(runs):
        wt = weight_of(fine_m[j], of_run(fine_tops, j))
        fine_sum.append(wt * fine_l[j])
        fine_num.append(wt * fine_n[j])
    tops = [coarse_tops, fine_tops]
    sums = [split_by_request(coarse_sum), split_by_request(fine_sum)]
    nums = [split_by_request(coarse_num), split_by_request(fine_num)]
    for r in range(requests):
        stat = jnp.zeros((heads, HEAD_DIM), F32)
        for kind in range(2):
            high = sums[kind][r].astype(BF16).astype(F32)
            for i, value in enumerate((tops[kind][r], high, sums[kind][r] - high)):
                stat = jnp.where(lane_id == 3 * kind + i, value, stat)
        for w in range(per_dev):
            part = slice(w * n, (w + 1) * n)
            row = w * requests + r
            for kind in range(2):
                gather_f[pl.ds(kind * kind_rows + row, n, stride=rows_out), :] = nums[kind][r][part]
            gather_f[pl.ds(unit + row, n, stride=rows_out), :] = stat[part]
    for d in range(n):
        send_buf[d] = gather_f[d * rows_out : (d + 1) * rows_out, :].astype(BF16)

    def p_copy(slot, peer):
        return pltpu.make_async_remote_copy(
            src_ref=send_buf.at[peer], dst_ref=recv_buf.at[slot], send_sem=p_send.at[peer],
            recv_sem=p_recv.at[slot], device_id={"seq": peer}, device_id_type=MESH,
        )

    for peer in peers:
        p_copy(me, peer).start()
    recv_buf[me] = send_buf[me]
    gates = jax.nn.sigmoid(gate_v[...])
    gate_lane = lax.broadcasted_iota(jnp.int32, gates.shape, 1)
    gate_col = [
        [
            jnp.sum(
                jnp.where(gate_lane == kind * heads + me * per_dev + w, gates, 0.0),
                axis=1, keepdims=True,
            )
            for w in range(per_dev)
        ]
        for kind in range(2)
    ]
    for peer in peers:
        p_copy(peer, peer).wait_recv()
    stats = [recv_buf[src, unit:, :].astype(F32) for src in range(n)]
    full = []
    for kind in range(2):
        tops = [s[:, 3 * kind : 3 * kind + 1] for s in stats]
        top = functools.reduce(jnp.maximum, tops)
        total = jnp.zeros((kind_rows, 1), F32)
        num = jnp.zeros((kind_rows, HEAD_DIM), F32)
        part = slice(kind * kind_rows, (kind + 1) * kind_rows)
        for src in range(n):
            weight = jnp.exp2(tops[src] - top)
            both = stats[src][:, 3 * kind + 1 : 3 * kind + 2] + stats[src][:, 3 * kind + 2 : 3 * kind + 3]
            total = total + weight * both
            num = num + weight * recv_buf[src, part, :].astype(F32)
        full.append(num / total)
    for w in range(per_dev):
        part = slice(w * requests, (w + 1) * requests)
        out_ref[:, w * HEAD_DIM : (w + 1) * HEAD_DIM] = (
            gate_col[0][w] * full[0][part] + gate_col[1][w] * full[1][part]
        ).astype(BF16)
    for peer in peers:
        q_copy(me, peer).wait_send()
        p_copy(me, peer).wait_send()


def per_device(queries, gate_logits, kv_pool, page_table, selected, lengths):
    n = lax.axis_size("seq")
    slots, page_len, width = kv_pool.shape
    requests, cols = queries.shape
    if cols % HEAD_DIM != 0 or n % 16 != 0:
        return per_device_plain(queries, gate_logits, kv_pool, page_table, selected, lengths)
    per_dev = cols // HEAD_DIM
    rows_out = 3 * per_dev * requests
    dma = pltpu.SemaphoreType.DMA
    return pl.pallas_call(
        functools.partial(fused_kernel, n),
        out_shape=jax.ShapeDtypeStruct((requests, cols), BF16),
        in_specs=[pl.BlockSpec(memory_space=pltpu.HBM)] * 6,
        out_specs=pl.BlockSpec(memory_space=pltpu.VMEM),
        scratch_shapes=[
            pltpu.VMEM(kv_pool.shape, BF16),
            pltpu.VMEM((n, requests, cols), BF16),
            pltpu.VMEM(gate_logits.shape, F32),
            pltpu.VMEM(page_table.shape, jnp.int32),
            pltpu.VMEM(selected.shape, jnp.int32),
            pltpu.SMEM(lengths.shape, jnp.int32),
            pltpu.VMEM((2, per_dev, n // 2 * requests, HEAD_DIM), F32),
            pltpu.VMEM((slots // RUN, per_dev * n, RUN * page_len), F32),
            pltpu.VMEM((slots, per_dev * n, HEAD_DIM), F32),
            pltpu.VMEM((slots, per_dev * n, HEAD_DIM), F32),
            pltpu.VMEM((n * rows_out, HEAD_DIM), F32),
            pltpu.VMEM((n, rows_out, HEAD_DIM), BF16),
            pltpu.VMEM((n, rows_out, HEAD_DIM), BF16),
            dma((slots // RUN,)),
            dma((5,)),
            dma((n,)),
            dma((n,)),
            dma((n,)),
            dma((n,)),
        ],
        compiler_params=pltpu.CompilerParams(
            collective_id=0, has_side_effects=True, vmem_limit_bytes=67043328
        ),
        name="paged_sparse_decode",
    )(queries, gate_logits, kv_pool, page_table, selected, lengths)


def solution(mesh):
    return jax.shard_map(
        per_device,
        mesh=mesh,
        in_specs=(
            P("grp", "seq"),
            P("grp", None),
            P(("grp", "seq"), None, None),
            P("grp", None),
            P("grp", None, None),
            P("grp"),
        ),
        out_specs=P("grp", "seq"),
        check_vma=False,
    )
```
